32 devices in a mesh: cell: 2 (over x), seq: 16 (over z, y, core).
Axes of the slice: x: 2, y: 2, z: 4, core: 2. Of those that a mesh axis runs over, the one named last changes fastest.
Arguments:
- queries: bfloat16 [128, 6144], P(('cell', 'seq')), parts along dimension 0, may hold values from -500 to 500
- keys: bfloat16 [256, 128, 1024], P(('cell', 'seq')), parts along dimension 0, may hold values from -6 to 6
- values: bfloat16 [256, 128, 1024], P(('cell', 'seq')), parts along dimension 0, may hold values from -6 to 6
- page_request: int32 [256], P(('cell', 'seq')), parts along dimension 0, may hold values from 0 to 63, as said below
- page_fill: int32 [256], P(('cell', 'seq')), parts along dimension 0, may hold values from 0 to 128
Outputs:
- attended: bfloat16 [128, 6144], P(('cell', 'seq')), parts along dimension 0
The draws below stay inside these ranges and needn't reach their ends.
There are 2 independent parts, one for each index of `cell`. The reference program is written for one: setup_inputs(seed, part) draws one part's arguments, and reference() takes and returns one part's arrays. A program takes and returns all parts, laid end to end along the dimension named above; each array names one. Nothing has to cross between parts.
Inputs may be any that keep to these rules, and one draw needn't show every extreme that they name: `page_request`: every request has at least one page with a live slot. Request r's home is index r // 4 of seq; among one device's pages, the requests of any one home are at most 2 distinct ones, and some device reaches that.
All inputs are finite; a program needn't handle non-finite values.
Results may differ from the reference program's by a relative error of at most 0.0035.
Values may be sent and summed in bfloat16 or wider, within the bound.
No kernel may reach another device: no remote copies, remote signals or barrier semaphores. Data moves between devices by JAX's collectives and lax.ppermute only.
A program may use at most 64 MiB of HBM per device.

```python
import jax
import jax.numpy as jnp
from jax import lax

HEADS = 48
KV_HEADS = 8
HEAD_DIM = 128
PAGE = 128
REQ_DEV = 4
PAGE_DEV = 8
GROUP = 6
REQUESTS = 64
PAGES = 128
N_SEQ = 16


def layout(key):
    base = jax.random.fold_in(key, 7)
    pairs = PAGE_DEV // 2
    order = jax.random.permutation(jax.random.fold_in(base, 1), N_SEQ)
    position = jax.random.permutation(jax.random.fold_in(base, 2), N_SEQ)
    rotation = jax.random.randint(jax.random.fold_in(base, 3), (N_SEQ,), 0, REQ_DEV)
    device_ids = jnp.arange(N_SEQ, dtype=jnp.int32)[:, None]
    pair_ids = jnp.arange(pairs, dtype=jnp.int32)[None, :]
    home = order[(position[device_ids] + pair_ids) % N_SEQ]
    first = (pair_ids + rotation[home]) % REQ_DEV
    second = jnp.where(pair_ids % 2 == 0, (first + 1) % REQ_DEV, first)
    owners = home[..., None] * REQ_DEV + jnp.stack([first, second], axis=-1)
    even = jnp.broadcast_to((pair_ids % 2 == 0)[..., None], (N_SEQ, pairs, 2))
    filled = jnp.clip(jax.random.randint(jax.random.fold_in(base, 4), (N_SEQ, pairs, 2), -40, PAGE + 1), 0, PAGE)
    filled = jnp.where(even, jnp.maximum(filled, 1), filled)
    owners = owners.reshape(N_SEQ, PAGE_DEV).astype(jnp.int32)
    filled = filled.reshape(N_SEQ, PAGE_DEV).astype(jnp.int32)
    shuffle_key = jax.random.fold_in(base, 5)

    def shuffle(index):
        return jax.random.permutation(jax.random.fold_in(shuffle_key, index), PAGE_DEV)
    perms = jax.vmap(shuffle)(jnp.arange(N_SEQ, dtype=jnp.int32))
    owners = jnp.take_along_axis(owners, perms, axis=1)
    filled = jnp.take_along_axis(filled, perms, axis=1)
    return (owners.reshape(PAGES), filled.reshape(PAGES))


def draw_page_request(key, part):
    return layout(key)[0]


def draw_page_fill(key, part):
    return layout(key)[1]


def draw_queries(key, part):
    base = jax.random.normal(jax.random.fold_in(key, 11), (REQUESTS, HEADS * HEAD_DIM), jnp.float32)
    base = jnp.clip(base, -6.0, 6.0)
    return base.astype(jnp.bfloat16)


def block_levels(key, dims, shards, least, top_value):
    level = 1.0
    for dim, parts in shards:
        steps = jax.random.uniform(jax.random.fold_in(jax.random.fold_in(key, 6), dim), (parts,), jnp.float32, least / len(shards), top_value / len(shards))
        level = level * jnp.repeat(jnp.exp(steps), dims[dim] // parts).reshape((-1,) + (1,) * (len(dims) - 1 - dim))
    return level


def bell_draw(rng, extent, spread, bound, shards=(), kind=jnp.bfloat16):
    drawn = spread * jax.random.normal(rng, extent, jnp.float32)
    if shards:
        drawn = drawn * block_levels(rng, extent, shards, -0.22, 0.18)
    return jnp.clip(drawn, -bound, bound).astype(kind)


def setup_inputs(seed: int = 0, part: int = 0) -> dict:
    splits = jax.random.split(jax.random.key(seed), 6)
    part_keys = jax.random.split(jax.random.fold_in(splits[5], part), 6)
    queries = draw_queries(jax.random.fold_in(jax.random.fold_in(splits[5], part), 71), part)
    keys = bell_draw(part_keys[1], (PAGES, PAGE, KV_HEADS * HEAD_DIM), 1.0, 6.0, ((0, 16),))
    values = bell_draw(part_keys[2], (PAGES, PAGE, KV_HEADS * HEAD_DIM), 1.0, 6.0, ((0, 16),))
    page_request = draw_page_request(jax.random.fold_in(jax.random.fold_in(splits[5], part), 71), part)
    page_fill = draw_page_fill(jax.random.fold_in(jax.random.fold_in(splits[5], part), 71), part)
    return {"queries": queries, "keys": keys, "values": values, "page_request": page_request, "page_fill": page_fill}


FLOOR = -30000.0


def device_partials(everyone, keys, values, page_request, page_fill):
    pages = keys.shape[0]
    chosen = jnp.take(everyone, page_request, axis=0).reshape(pages, KV_HEADS, GROUP, HEAD_DIM)
    keyed = keys.reshape(pages, PAGE, KV_HEADS, HEAD_DIM)
    valued = values.reshape(pages, PAGE, KV_HEADS, HEAD_DIM)
    scores = jnp.einsum('pkgd,ptkd->pkgt', chosen.astype(jnp.float32), keyed.astype(jnp.float32)) * (HEAD_DIM ** -0.5)
    live = (lax.broadcasted_iota(jnp.int32, (pages, PAGE), 1) < page_fill[:, None])[:, None, None, :]
    page_max = jnp.max(jnp.where(live, scores, FLOOR), axis=3)
    weights = jnp.where(live, jnp.exp(scores - page_max[..., None]), 0.0).astype(jnp.bfloat16)
    page_sum = jnp.sum(weights.astype(jnp.float32), axis=3).reshape(pages, HEADS)
    page_acc = jnp.einsum('pkgt,ptkd->pkgd', weights.astype(jnp.float32), valued.astype(jnp.float32)).reshape(pages, HEADS, HEAD_DIM)
    page_max = page_max.reshape(pages, HEADS)
    member = page_request[None, :] == lax.broadcasted_iota(jnp.int32, (REQUESTS, pages), 0)
    local_max = jnp.max(jnp.where(member[:, :, None], page_max[None], FLOOR), axis=1)
    factor = jnp.where(member[:, :, None], jnp.exp(page_max[None] - local_max[:, None, :]), 0.0)
    local_sum = jnp.sum(factor * page_sum[None], axis=1)
    local_acc = jnp.einsum('rph,phd->rhd', factor, page_acc, precision=lax.Precision.HIGHEST)
    partial_value = (local_acc / jnp.maximum(local_sum, 1.0)[..., None]).astype(jnp.bfloat16)
    return partial_value, local_max, local_sum


def reference(queries, keys, values, page_request, page_fill):
    width = KV_HEADS * HEAD_DIM
    keys_dev = keys.reshape(N_SEQ, PAGE_DEV, PAGE, width)
    values_dev = values.reshape(N_SEQ, PAGE_DEV, PAGE, width)
    request_dev = page_request.reshape(N_SEQ, PAGE_DEV)
    fill_dev = page_fill.reshape(N_SEQ, PAGE_DEV)

    def one_device(items):
        return device_partials(queries, items[0], items[1], items[2], items[3])

    partial_value, local_max, local_sum = lax.map(one_device, (keys_dev, values_dev, request_dev, fill_dev))
    top = jnp.max(local_max, axis=0)
    share = local_sum * jnp.exp(local_max - top[None])

    def accumulate(total, items):
        return total + items[0][..., None] * items[1].astype(jnp.float32), None

    numer, _ = lax.scan(accumulate, jnp.zeros((REQUESTS, HEADS, HEAD_DIM), jnp.float32), (share, partial_value))
    denom = jnp.sum(share, axis=0)
    return (numer / denom[..., None]).reshape(REQUESTS, HEADS * HEAD_DIM).astype(jnp.bfloat16)
```

```python
import functools

import jax
import jax.numpy as jnp
from jax import lax
from jax.experimental import pallas as pl
from jax.experimental.pallas import tpu as pltpu
from jax.sharding import PartitionSpec as P

HEADS = 48
KV_HEADS = 8
HEAD_DIM = 128
GROUP = 6
LANES = 128
HALF = LANES // 2

FLOOR = -30000.0
SLOTS = 2
STATS = 8
ROWS = SLOTS * HEADS + STATS


def exchange(x, step, count):
    return lax.ppermute(x, "seq", [(i, i ^ step) for i in range(count)])


def gather_queries(queries, count):
    far = [4 * k for k in range(count // 4 - 1, 0, -1)]
    pieces = {0: queries}
    for step in far:
        pieces[step] = exchange(queries, step, count)
    for step in [0] + far[::-1]:
        pieces[step ^ 2] = exchange(pieces[step], 2, count)
    for step in list(pieces):
        pieces[step ^ 1] = exchange(pieces[step], 1, count)
    return [pieces[k] for k in range(count)]


def split3(x):
    high = x.astype(jnp.bfloat16)
    rest = x - high.astype(jnp.float32)
    middle = rest.astype(jnp.bfloat16)
    low = (rest - middle.astype(jnp.float32)).astype(jnp.bfloat16)
    return [high.astype(jnp.float32), middle.astype(jnp.float32), low.astype(jnp.float32)]


def attend_kernel(blocks, by_xor, request, fill, *refs):
    query_refs, (keys, values, send, held, spread, accs) = refs[:blocks], refs[blocks:]
    pages, page_len, _ = keys.shape
    homes, req_dev, width = held.shape
    me = lax.axis_index("seq") if by_xor else 0
    if by_xor:
        for k in range(blocks):
            held[k] = query_refs[k][...]
    else:
        held[...] = query_refs[0][...]
    lane = lax.broadcasted_iota(jnp.int32, (HEADS, LANES), 1)
    kv_of = lax.broadcasted_iota(jnp.int32, (HEADS, LANES), 0) // GROUP
    owner = [request[p] // req_dev for p in range(pages)]
    local = [request[p] % req_dev for p in range(pages)]
    maxima = jnp.full((HEADS, LANES), FLOOR, jnp.float32)
    sums = jnp.zeros((HEADS, LANES), jnp.float32)
    names = jnp.full((HEADS, LANES), -1, jnp.int32)
    for p in range(pages):
        block = held[owner[p] ^ me].astype(jnp.float32)
        for h in range(HEADS):
            spread[p, req_dev * h : req_dev * (h + 1), :] = block[:, LANES * h : LANES * (h + 1)]
        query = spread[p, pl.ds(local[p], HEADS, stride=req_dev), :].astype(jnp.bfloat16)
        zero = jnp.zeros_like(query)
        wide = jnp.concatenate([jnp.where(kv_of == k, query, zero) for k in range(KV_HEADS)], axis=1)
        scores = lax.dot_general(
            wide, keys[p], (((1,), (1,)), ((), ())), preferred_element_type=jnp.float32
        ) * HEAD_DIM ** (-0.5)
        live = lax.broadcasted_iota(jnp.int32, (HEADS, page_len), 1) < fill[p]
        peak = jnp.max(jnp.where(live, scores, FLOOR), axis=1, keepdims=True)
        weights = jnp.where(live, jnp.exp(scores - peak), 0.0).astype(jnp.bfloat16)
        total = jnp.sum(weights.astype(jnp.float32), axis=1, keepdims=True)
        mixed = lax.dot_general(
            weights, values[p], (((1,), (0,)), ((), ())), preferred_element_type=jnp.float32
        )
        acc = jnp.zeros((HEADS, HEAD_DIM), jnp.float32)
        for k in range(KV_HEADS):
            acc = jnp.where(kv_of == k, mixed[:, LANES * k : LANES * (k + 1)], acc)
        accs[p] = acc
        maxima = jnp.where(lane == p, peak, maxima)
        sums = jnp.where(lane == p, total, sums)
        names = jnp.where(lane == p, request[p], names)

    send[...] = jnp.zeros_like(send)
    row = lax.broadcasted_iota(jnp.int32, (homes, STATS, LANES), 1)
    send[:, SLOTS * HEADS :, :] = jnp.where(row == 6, -1.0, 0.0).astype(send.dtype)

    leader = []
    stats = jnp.zeros((HEADS, LANES), jnp.float32)
    for q in range(pages):
        earlier = [request[p] == request[q] for p in range(q)]
        leader.append(jnp.logical_not(functools.reduce(jnp.logical_or, earlier, jnp.bool_(False))))
        rank = jnp.int32(0)
        for p in range(q):
            rank += jnp.where(jnp.logical_and(leader[p], owner[p] == owner[q]), 1, 0)
        same = names == request[q]
        slot_max = jnp.max(jnp.where(same, maxima, FLOOR), axis=1, keepdims=True)
        factor = jnp.where(same, jnp.exp(maxima - slot_max), 0.0)
        slot_sum = jnp.sum(factor * sums, axis=1, keepdims=True)
        stats = jnp.where(lane == q, slot_max, stats)
        stats = jnp.where(lane == pages + q, slot_sum, stats)

        @pl.when(leader[q])
        def _():
            merged = factor[:, q : q + 1] * accs[q]
            for p in range(q + 1, pages):
                merged += factor[:, p : p + 1] * accs[p]
            part = (merged / jnp.maximum(slot_sum, 1.0)).astype(send.dtype)
            start = pl.multiple_of(jnp.minimum(rank, SLOTS - 1) * HEADS, HEADS)
            send[owner[q], pl.ds(start, HEADS), :] = part

    flat = jnp.transpose(jnp.concatenate([stats, jnp.zeros((LANES - HEADS, LANES), jnp.float32)], axis=0))
    for q in range(pages):
        rank = jnp.int32(0)
        for p in range(q):
            rank += jnp.where(jnp.logical_and(leader[p], owner[p] == owner[q]), 1, 0)
        lines = split3(flat[q : q + 1, :HALF]) + split3(flat[pages + q : pages + q + 1, :HALF])
        lines.append(jnp.full((1, HALF), local[q], jnp.int32).astype(jnp.float32))
        lines.append(jnp.zeros((1, HALF), jnp.float32))
        tile = jnp.concatenate(lines, axis=0).astype(send.dtype)
        for slot in range(SLOTS):

            @pl.when(jnp.logical_and(leader[q], rank == slot))
            def _():
                send[owner[q], SLOTS * HEADS :, HALF * slot : HALF * (slot + 1)] = tile


def attend(pieces, by_xor, count, keys, values, page_request, page_fill, req_dev):
    pages = keys.shape[0]
    width = HEADS * HEAD_DIM
    vmem = pl.BlockSpec(memory_space=pltpu.VMEM)
    smem = pl.BlockSpec(memory_space=pltpu.SMEM)
    return pl.pallas_call(
        functools.partial(attend_kernel, len(pieces), by_xor),
        name="attend",
        out_shape=jax.ShapeDtypeStruct((count, ROWS, LANES), jnp.bfloat16),
        in_specs=[smem, smem] + [vmem] * (len(pieces) + 2),
        out_specs=vmem,
        scratch_shapes=[
            pltpu.VMEM((count, req_dev, width), jnp.bfloat16),
            pltpu.VMEM((pages, HEADS * req_dev, LANES), jnp.float32),
            pltpu.VMEM((pages, HEADS, HEAD_DIM), jnp.float32),
        ],
        compiler_params=pltpu.CompilerParams(vmem_limit_bytes=32 * 2**20),
    )(page_request, page_fill, *pieces, keys, values)


def merge_kernel(got, out, accs):
    homes = got.shape[0]
    req_dev = out.shape[0]
    stats = got[:, SLOTS * HEADS :, :].astype(jnp.float32)
    peak = stats[:, 0, :] + stats[:, 1, :] + stats[:, 2, :]
    total = stats[:, 3, :] + stats[:, 4, :] + stats[:, 5, :]
    name = stats[:, 6, :]
    top = jnp.full(peak.shape, FLOOR, jnp.float32)
    for r in range(req_dev):
        best = jnp.max(jnp.where(name == r, peak, FLOOR), axis=0, keepdims=True)
        best = jnp.maximum(best, pltpu.roll(best, HALF, 1))
        top = jnp.where(name == r, best, top)
    share = jnp.where(name >= 0.0, total * jnp.exp(peak - top), 0.0)
    denom = jnp.ones(peak.shape, jnp.float32)
    for r in range(req_dev):
        whole = jnp.sum(jnp.where(name == r, share, 0.0), axis=0, keepdims=True)
        whole = whole + pltpu.roll(whole, HALF, 1)
        denom = jnp.where(name == r, whole, denom)
    weight = jnp.where(name >= 0.0, share / denom, 0.0)
    pad = jnp.zeros((LANES - homes, LANES), jnp.float32)
    turned = jnp.transpose(jnp.concatenate([weight, pad], axis=0))
    sums = [jnp.zeros((HEADS, HEAD_DIM), jnp.float32) for _ in range(req_dev)]
    for s in range(homes):
        for slot in range(SLOTS):
            part = got[s, HEADS * slot : HEADS * (slot + 1), :].astype(jnp.float32)
            part = part * turned[HALF * slot : HALF * slot + HEADS, s : s + 1]
            which = jnp.broadcast_to(name[s : s + 1, HALF * slot : HALF * slot + 1], part.shape)
            for r in range(req_dev):
                sums[r] = sums[r] + jnp.where(which == r, part, 0.0)
    for r in range(req_dev):
        accs[HEADS * r : HEADS * (r + 1), :] = sums[r]
    for h in range(HEADS):
        out[:, LANES * h : LANES * (h + 1)] = accs[pl.ds(h, req_dev, stride=HEADS), :].astype(out.dtype)


def merge(got, req_dev):
    vmem = pl.BlockSpec(memory_space=pltpu.VMEM)
    return pl.pallas_call(
        merge_kernel,
        name="merge",
        out_shape=jax.ShapeDtypeStruct((req_dev, HEADS * HEAD_DIM), jnp.bfloat16),
        in_specs=[vmem],
        out_specs=vmem,
        scratch_shapes=[pltpu.VMEM((req_dev * HEADS, HEAD_DIM), jnp.float32)],
        compiler_params=pltpu.CompilerParams(vmem_limit_bytes=32 * 2**20),
    )(got)


def body(queries, keys, values, page_request, page_fill):
    count = lax.axis_size("seq")
    req_dev = queries.shape[0]
    by_xor = count in (4, 8, 16)
    if by_xor:
        pieces = gather_queries(queries, count)
    else:
        pieces = [lax.all_gather(queries, "seq", axis=0)]
    send = attend(pieces, by_xor, count, keys, values, page_request, page_fill, req_dev)
    got = lax.all_to_all(send, "seq", split_axis=0, concat_axis=0, tiled=True)
    return merge(got, req_dev)


def solution(mesh):
    placed = (
        P(("cell", "seq"), None),
        P(("cell", "seq"), None, None),
        P(("cell", "seq"), None, None),
        P(("cell", "seq")),
        P(("cell", "seq")),
    )
    return jax.shard_map(
        body, mesh=mesh, in_specs=placed, out_specs=P(("cell", "seq"), None), check_vma=False
    )
```

```python
import functools

import jax
import jax.numpy as jnp
from jax import lax
from jax.experimental import pallas as pl
from jax.experimental.pallas import tpu as pltpu
from jax.sharding import PartitionSpec as P

HEADS = 48
KV_HEADS = 8
HEAD_DIM = 128
GROUP = 6
LANES = 128
HALF = LANES // 2

FLOOR = -30000.0
SLOTS = 2
STATS = 8
ROWS = SLOTS * HEADS + STATS

PASS_FLOPS = 20_000_000_000


def exchange(x, step, count):
    return lax.ppermute(x, "seq", [(i, i ^ step) for i in range(count)])


def gather_queries(queries, count):
    far = [4 * k for k in range(count // 4 - 1, 0, -1)]
    pieces = {0: queries}
    for step in far:
        pieces[step] = exchange(queries, step, count)
    for step in [0] + far[::-1]:
        pieces[step ^ 2] = exchange(pieces[step], 2, count)
    for step in list(pieces):
        pieces[step ^ 1] = exchange(pieces[step], 1, count)
    return [pieces[k] for k in range(count)]


def pass_kernel(source, target):
    del source, target


def pass_on(x):
    spec = pl.BlockSpec(memory_space=pltpu.VMEM)
    return pl.pallas_call(
        pass_kernel,
        name="pass_on",
        out_shape=jax.ShapeDtypeStruct(x.shape, x.dtype),
        in_specs=[spec],
        out_specs=spec,
        input_output_aliases={0: 0},
        compiler_params=pltpu.CompilerParams(vmem_limit_bytes=16 * 2**20),
        cost_estimate=pl.CostEstimate(flops=PASS_FLOPS, bytes_accessed=0, transcendentals=0),
    )(x)


def split3(x):
    high = x.astype(jnp.bfloat16).astype(jnp.float32)
    middle = (x - high).astype(jnp.bfloat16).astype(jnp.float32)
    low = (x - high - middle).astype(jnp.bfloat16).astype(jnp.float32)
    return [high, middle, low]


def attend_kernel(blocks, by_xor, request, fill, *refs):
    query_refs, (keys, values, send, held, spread, accs, rows) = refs[:blocks], refs[blocks:]
    pages, page_len, _ = keys.shape
    homes, req_dev, width = held.shape
    me = lax.axis_index("seq") if by_xor else 0
    if by_xor:
        for k in range(blocks):
            held[k] = query_refs[k][...]
    else:
        held[...] = query_refs[0][...]
    lane = lax.broadcasted_iota(jnp.int32, (HEADS, LANES), 1)
    kv_of = lax.broadcasted_iota(jnp.int32, (HEADS, LANES), 0) // GROUP
    owner = [request[p] // req_dev for p in range(pages)]
    local = [request[p] % req_dev for p in range(pages)]
    same = [[request[p] == request[q] for q in range(pages)] for p in range(pages)]
    first, leader, rank = [], [], []
    for p in range(pages):
        lead = jnp.int32(p)
        for q in range(p - 1, -1, -1):
            lead = jnp.where(same[p][q], q, lead)
        first.append(lead)
        leader.append(lead == p)
    for p in range(pages):
        before = jnp.int32(0)
        for q in range(pages):
            other = jnp.logical_and(leader[q], owner[q] == owner[p])
            before += jnp.where(jnp.logical_and(other, q < first[p]), 1, 0)
        rank.append(jnp.minimum(before, SLOTS - 1))

    for p in range(pages):
        block = held[owner[p] ^ me].astype(jnp.float32)
        for h in range(HEADS):
            spread[p, req_dev * h : req_dev * (h + 1), :] = block[:, LANES * h : LANES * (h + 1)]
        query = spread[p, pl.ds(local[p], HEADS, stride=req_dev), :].astype(jnp.bfloat16)
        zero = jnp.zeros_like(query)
        wide = jnp.concatenate([jnp.where(kv_of == k, query, zero) for k in range(KV_HEADS)], axis=1)
        accs[p] = lax.dot_general(
            wide, keys[p], (((1,), (1,)), ((), ())), preferred_element_type=jnp.float32
        ) * HEAD_DIM ** (-0.5)

    peaks = []
    for p in range(pages):
        live = lax.broadcasted_iota(jnp.int32, (HEADS, page_len), 1) < fill[p]
        peaks.append(jnp.max(jnp.where(live, accs[p], FLOOR), axis=1, keepdims=True))
    tops = []
    for p in range(pages):
        top = peaks[p]
        for q in range(pages):
            if q != p:
                top = jnp.maximum(top, jnp.where(same[p][q], peaks[q], FLOOR))
        tops.append(top)
    heavy, totals = [], []
    for p in range(pages):
        live = lax.broadcasted_iota(jnp.int32, (HEADS, page_len), 1) < fill[p]
        weights = jnp.where(live, jnp.exp(accs[p] - tops[p]), 0.0).astype(jnp.bfloat16)
        heavy.append(weights)
        totals.append(jnp.sum(weights.astype(jnp.float32), axis=1, keepdims=True))
    sums = []
    for p in range(pages):
        total = totals[p]
        for q in range(pages):
            if q != p:
                total = total + jnp.where(same[p][q], totals[q], 0.0)
        sums.append(total)

    accs[...] = jnp.zeros_like(accs)
    for p in range(pages):
        mixed = lax.dot_general(
            heavy[p], values[p], (((1,), (0,)), ((), ())), preferred_element_type=jnp.float32
        )
        acc = mixed[:, :LANES]
        for k in range(1, KV_HEADS):
            acc = jnp.where(kv_of == k, mixed[:, LANES * k : LANES * (k + 1)], acc)
        accs[first[p]] += acc

    send[...] = jnp.zeros_like(send)
    row = lax.broadcasted_iota(jnp.int32, (homes, STATS, LANES), 1)
    send[:, SLOTS * HEADS :, :] = jnp.where(row == 6, -1.0, 0.0).astype(send.dtype)
    for p in range(pages):
        part = (accs[first[p]] / jnp.maximum(sums[p], 1.0)).astype(send.dtype)
        send[owner[p], pl.ds(pl.multiple_of(rank[p] * HEADS, HEADS), HEADS), :] = part

    stats = jnp.zeros((HEADS, LANES), jnp.float32)
    for p in range(pages):
        stats = jnp.where(lane == p, tops[p], stats)
        stats = jnp.where(lane == pages + p, sums[p], stats)
    pad = jnp.zeros((LANES - HEADS, LANES), jnp.float32)
    flat = jnp.transpose(jnp.concatenate([stats, pad], axis=0))
    lines = split3(flat[:pages]) + split3(flat[pages : 2 * pages])
    page = lax.broadcasted_iota(jnp.int32, (pages, LANES), 0)
    name = jnp.zeros((pages, LANES), jnp.int32)
    for p in range(pages):
        name = jnp.where(page == p, local[p], name)
    lines.append(name.astype(jnp.float32))
    rows[...] = jnp.zeros_like(rows)
    for i, line in enumerate(lines):
        rows[pl.ds(i, pages, stride=STATS), :] = line + pltpu.roll(line, HALF, 1) if i < 6 else line
    high = lax.broadcasted_iota(jnp.int32, (STATS, LANES), 1) // HALF
    for p in range(pages):
        tile = rows[STATS * p : STATS * (p + 1), :]
        old = send[owner[p], SLOTS * HEADS :, :].astype(jnp.float32)
        send[owner[p], SLOTS * HEADS :, :] = jnp.where(high == rank[p], tile, old).astype(send.dtype)


def attend(pieces, by_xor, count, keys, values, page_request, page_fill, req_dev):
    pages = keys.shape[0]
    width = HEADS * HEAD_DIM
    vmem = pl.BlockSpec(memory_space=pltpu.VMEM)
    smem = pl.BlockSpec(memory_space=pltpu.SMEM)
    return pl.pallas_call(
        functools.partial(attend_kernel, len(pieces), by_xor),
        name="attend",
        out_shape=jax.ShapeDtypeStruct((count, ROWS, LANES), jnp.bfloat16),
        in_specs=[smem, smem] + [vmem] * (len(pieces) + 2),
        out_specs=vmem,
        scratch_shapes=[
            pltpu.VMEM((count, req_dev, width), jnp.bfloat16),
            pltpu.VMEM((pages, HEADS * req_dev, LANES), jnp.float32),
            pltpu.VMEM((pages, HEADS, HEAD_DIM), jnp.float32),
            pltpu.VMEM((pages * STATS, LANES), jnp.float32),
        ],
        compiler_params=pltpu.CompilerParams(vmem_limit_bytes=32 * 2**20),
    )(page_request, page_fill, *pieces, keys, values)


def merge_kernel(got, out, accs):
    homes = got.shape[0]
    req_dev = out.shape[0]
    stats = got[:, SLOTS * HEADS :, :].astype(jnp.float32)
    peak = stats[:, 0, :] + stats[:, 1, :] + stats[:, 2, :]
    total = stats[:, 3, :] + stats[:, 4, :] + stats[:, 5, :]
    name = stats[:, 6, :]
    top = jnp.full(peak.shape, FLOOR, jnp.float32)
    for r in range(req_dev):
        best = jnp.max(jnp.where(name == r, peak, FLOOR), axis=0, keepdims=True)
        best = jnp.maximum(best, pltpu.roll(best, HALF, 1))
        top = jnp.where(name == r, best, top)
    share = jnp.where(name >= 0.0, total * jnp.exp(peak - top), 0.0)
    denom = jnp.ones(peak.shape, jnp.float32)
    for r in range(req_dev):
        whole = jnp.sum(jnp.where(name == r, share, 0.0), axis=0, keepdims=True)
        whole = whole + pltpu.roll(whole, HALF, 1)
        denom = jnp.where(name == r, whole, denom)
    weight = jnp.where(name >= 0.0, share / denom, 0.0)
    pad = jnp.zeros((LANES - homes, LANES), jnp.float32)
    turned = jnp.transpose(jnp.concatenate([weight, pad], axis=0))
    sums = [jnp.zeros((HEADS, HEAD_DIM), jnp.float32) for _ in range(req_dev)]
    for s in range(homes):
        for slot in range(SLOTS):
            part = got[s, HEADS * slot : HEADS * (slot + 1), :].astype(jnp.float32)
            part = part * turned[HALF * slot : HALF * slot + HEADS, s : s + 1]
            which = jnp.broadcast_to(name[s : s + 1, HALF * slot : HALF * slot + 1], part.shape)
            for r in range(req_dev):
                sums[r] = sums[r] + jnp.where(which == r, part, 0.0)
    for r in range(req_dev):
        accs[HEADS * r : HEADS * (r + 1), :] = sums[r]
    for h in range(HEADS):
        out[:, LANES * h : LANES * (h + 1)] = accs[pl.ds(h, req_dev, stride=HEADS), :].astype(out.dtype)


def merge(got, req_dev):
    vmem = pl.BlockSpec(memory_space=pltpu.VMEM)
    return pl.pallas_call(
        merge_kernel,
        name="merge",
        out_shape=jax.ShapeDtypeStruct((req_dev, HEADS * HEAD_DIM), jnp.bfloat16),
        in_specs=[vmem],
        out_specs=vmem,
        scratch_shapes=[pltpu.VMEM((req_dev * HEADS, HEAD_DIM), jnp.float32)],
        compiler_params=pltpu.CompilerParams(vmem_limit_bytes=32 * 2**20),
    )(got)


def body(queries, keys, values, page_request, page_fill):
    count = lax.axis_size("seq")
    req_dev = queries.shape[0]
    by_xor = count in (4, 8, 16)
    if by_xor:
        pieces = gather_queries(queries, count)
        pieces[count // 2] = pass_on(pieces[count // 2])
    else:
        pieces = [lax.all_gather(queries, "seq", axis=0)]
    send = attend(pieces, by_xor, count, keys, values, page_request, page_fill, req_dev)
    got = lax.all_to_all(send, "seq", split_axis=0, concat_axis=0, tiled=True)
    return merge(got, req_dev)


def solution(mesh):
    placed = (
        P(("cell", "seq"), None),
        P(("cell", "seq"), None, None),
        P(("cell", "seq"), None, None),
        P(("cell", "seq")),
        P(("cell", "seq")),
    )
    return jax.shard_map(
        body, mesh=mesh, in_specs=placed, out_specs=P(("cell", "seq"), None), check_vma=False
    )
```

```python
import functools

import jax
import jax.numpy as jnp
from jax import lax
from jax.experimental import pallas as pl
from jax.experimental.pallas import tpu as pltpu
from jax.sharding import PartitionSpec as P

HEADS = 48
KV_HEADS = 8
HEAD_DIM = 128
GROUP = 6
LANES = 128
HALF = LANES // 2

FLOOR = -30000.0
LAYER = 4
PASS_FLOPS = 20_000_000_000


def exchange(x, step, count):
    return lax.ppermute(x, "seq", [(i, i ^ step) for i in range(count)])


def gather_queries(queries, count):
    far = [4 * k for k in range(count // 4 - 1, 0, -1)]
    pieces = {0: queries}
    for step in far:
        pieces[step] = exchange(queries, step, count)
    for step in [0] + far[::-1]:
        pieces[step ^ 2] = exchange(pieces[step], 2, count)
    for step in list(pieces):
        pieces[step ^ 1] = exchange(pieces[step], 1, count)
    return [pieces[k] for k in range(count)]


def pass_kernel(source, target):
    del source, target


def pass_on(x):
    spec = pl.BlockSpec(memory_space=pltpu.VMEM)
    return pl.pallas_call(
        pass_kernel,
        name="pass_on",
        out_shape=jax.ShapeDtypeStruct(x.shape, x.dtype),
        in_specs=[spec],
        out_specs=spec,
        input_output_aliases={0: 0},
        compiler_params=pltpu.CompilerParams(vmem_limit_bytes=16 * 2**20),
        cost_estimate=pl.CostEstimate(flops=PASS_FLOPS, bytes_accessed=0, transcendentals=0),
    )(x)


def split3(x):
    high = x.astype(jnp.bfloat16).astype(jnp.float32)
    middle = (x - high).astype(jnp.bfloat16).astype(jnp.float32)
    low = (x - high - middle).astype(jnp.bfloat16).astype(jnp.float32)
    return [high, middle, low]


def attend_kernel(blocks, by_xor, request, fill, *refs):
    query_refs, (keys, values, send, held, spread, accs) = refs[:blocks], refs[blocks:]
    pages, page_len, _ = keys.shape
    homes, req_dev, width = held.shape
    me = lax.axis_index("seq") if by_xor else 0
    if by_xor:
        for k in range(blocks):
            held[k] = query_refs[k][...]
    else:
        held[...] = query_refs[0][...]
    lane = lax.broadcasted_iota(jnp.int32, (HEADS, LANES), 1)
    kv_of = lax.broadcasted_iota(jnp.int32, (HEADS, LANES), 0) // GROUP

    for p in range(pages):
        block = held[(request[p] // req_dev) ^ me].astype(jnp.float32)
        for h in range(HEADS):
            spread[p, req_dev * h : req_dev * (h + 1), :] = block[:, LANES * h : LANES * (h + 1)]
        query = spread[p, pl.ds(request[p] % req_dev, HEADS, stride=req_dev), :].astype(jnp.bfloat16)
        zero = jnp.zeros_like(query)
        wide = jnp.concatenate([jnp.where(kv_of == k, query, zero) for k in range(KV_HEADS)], axis=1)
        accs[p] = lax.dot_general(
            wide, keys[p], (((1,), (1,)), ((), ())), preferred_element_type=jnp.float32
        ) * HEAD_DIM ** (-0.5)

    heavy, totals = [], []
    stats = jnp.zeros((HEADS, LANES), jnp.float32)
    for p in range(pages):
        scores = accs[p]
        live = lax.broadcasted_iota(jnp.int32, (HEADS, page_len), 1) < fill[p]
        peak = jnp.max(jnp.where(live, scores, FLOOR), axis=1, keepdims=True)
        weights = jnp.where(live, jnp.exp(scores - peak), 0.0).astype(jnp.bfloat16)
        total = jnp.sum(weights.astype(jnp.float32), axis=1, keepdims=True)
        heavy.append(weights)
        totals.append(total)
        stats = jnp.where(lane == p, peak, stats)
        stats = jnp.where(lane == pages + p, total, stats)
    high, middle, low = split3(stats)
    stats = high + pltpu.roll(middle, 2 * pages, 1) + pltpu.roll(low, 4 * pages, 1)
    send[HEADS * pages :, :] = stats.astype(send.dtype)

    for p in range(pages):
        mixed = lax.dot_general(
            heavy[p], values[p], (((1,), (0,)), ((), ())), preferred_element_type=jnp.float32
        )
        acc = mixed[:, :LANES]
        for k in range(1, KV_HEADS):
            acc = jnp.where(kv_of == k, mixed[:, LANES * k : LANES * (k + 1)], acc)
        send[HEADS * p : HEADS * (p + 1), :] = (acc / jnp.maximum(totals[p], 1.0)).astype(send.dtype)


def attend(pieces, by_xor, count, keys, values, page_request, page_fill, req_dev):
    pages = keys.shape[0]
    width = HEADS * HEAD_DIM
    vmem = pl.BlockSpec(memory_space=pltpu.VMEM)
    smem = pl.BlockSpec(memory_space=pltpu.SMEM)
    return pl.pallas_call(
        functools.partial(attend_kernel, len(pieces), by_xor),
        name="attend",
        out_shape=jax.ShapeDtypeStruct(((pages + 1) * HEADS, LANES), jnp.bfloat16),
        in_specs=[smem, smem] + [vmem] * (len(pieces) + 2),
        out_specs=vmem,
        scratch_shapes=[
            pltpu.VMEM((count, req_dev, width), jnp.bfloat16),
            pltpu.VMEM((pages, HEADS * req_dev, LANES), jnp.float32),
            pltpu.VMEM((pages, HEADS, HEAD_DIM), jnp.float32),
        ],
        compiler_params=pltpu.CompilerParams(vmem_limit_bytes=32 * 2**20),
    )(page_request, page_fill, *pieces, keys, values)


def layer_kernel(req_dev, *refs):
    requests, rows, outs, sums = refs[:LAYER], refs[LAYER : 2 * LAYER], refs[2 * LAYER : -1], refs[-1]
    pages = rows[0].shape[0] // HEADS - 1
    homes = len(outs)
    slots = homes * req_dev
    me = lax.axis_index("seq")
    lane = lax.broadcasted_iota(jnp.int32, (HEADS, LANES), 1)
    sums[...] = jnp.zeros_like(sums)

    place, peaks, totals = [], jnp.full((HEADS, LANES), FLOOR, jnp.float32), jnp.zeros((HEADS, LANES), jnp.float32)
    where = jnp.full((1, LANES), -1, jnp.int32)
    for s in range(LAYER):
        stats = rows[s][HEADS * pages :, :].astype(jnp.float32)
        stats = stats + pltpu.roll(stats, LANES - 2 * pages, 1) + pltpu.roll(stats, LANES - 4 * pages, 1)
        inside = jnp.logical_and(lane >= pages * s, lane < pages * (s + 1))
        peaks = jnp.where(inside, pltpu.roll(stats, (pages * s) % LANES, 1), peaks)
        totals = jnp.where(inside, pltpu.roll(stats, (pages * (s - 1)) % LANES, 1), totals)
        for p in range(pages):
            apart = (requests[s][p] // req_dev) ^ me
            mine = apart % LAYER == 0
            place.append(jnp.where(mine, apart // LAYER * req_dev + requests[s][p] % req_dev, slots))
            where = jnp.where(lane[:1] == len(place) - 1, place[-1], where)

    tops = jnp.full((HEADS, LANES), FLOOR, jnp.float32)
    slot_tops = jnp.full((HEADS, LANES), FLOOR, jnp.float32)
    for i, at in enumerate(place):
        peak = peaks[:, i : i + 1]
        tops = jnp.maximum(tops, jnp.where(where == at, peak, FLOOR))
        slot_tops = jnp.maximum(slot_tops, jnp.where(lane == at, peak, FLOOR))
    shares = totals * jnp.exp(peaks - tops)
    wholes = jnp.zeros((HEADS, LANES), jnp.float32)
    slot_wholes = jnp.zeros((HEADS, LANES), jnp.float32)
    for i, at in enumerate(place):
        share = shares[:, i : i + 1]
        wholes = wholes + jnp.where(where == at, share, 0.0)
        slot_wholes = slot_wholes + jnp.where(lane == at, share, 0.0)
    shares = shares / jnp.maximum(wholes, 1.0)
    for i, at in enumerate(place):
        s, p = divmod(i, pages)
        sums[at] += rows[s][HEADS * p : HEADS * (p + 1), :].astype(jnp.float32) * shares[:, i : i + 1]

    pad = jnp.zeros((LANES - HEADS, LANES), jnp.float32)
    parts = []
    for table in (slot_tops, slot_wholes):
        flat = jnp.transpose(jnp.concatenate([table, pad], axis=0))
        parts += split3(flat[:slots])
    for k in range(homes):
        for r in range(req_dev):
            outs[k][HEADS * r : HEADS * (r + 1), :] = sums[req_dev * k + r].astype(outs[k].dtype)
        lines = []
        for part in parts:
            block = part[req_dev * k : req_dev * (k + 1)]
            block = jnp.concatenate([block, jnp.zeros((8 - req_dev, LANES), jnp.float32)], axis=0)
            lines.append(block + pltpu.roll(pltpu.roll(block, 8 - req_dev // 2, 0), HALF, 1))
        tail = [line[: req_dev // 2] for line in lines]
        spare = outs[k].shape[0] - HEADS * req_dev - 3 * req_dev
        if spare:
            tail.append(jnp.zeros((spare, LANES), jnp.float32))
        outs[k][HEADS * req_dev :, :] = jnp.concatenate(tail, axis=0).astype(outs[k].dtype)


def layer_merge(requests, rows, homes, req_dev):
    vmem = pl.BlockSpec(memory_space=pltpu.VMEM)
    smem = pl.BlockSpec(memory_space=pltpu.SMEM)
    height = HEADS * req_dev + -(-3 * req_dev // 8) * 8
    return pl.pallas_call(
        functools.partial(layer_kernel, req_dev),
        name="layer_merge",
        out_shape=[jax.ShapeDtypeStruct((height, LANES), jnp.bfloat16)] * homes,
        in_specs=[smem] * LAYER + [vmem] * LAYER,
        out_specs=[vmem] * homes,
        scratch_shapes=[pltpu.VMEM((homes * req_dev + 1, HEADS, HEAD_DIM), jnp.float32)],
        compiler_params=pltpu.CompilerParams(vmem_limit_bytes=16 * 2**20),
    )(*requests, *rows)


def home_kernel(*refs):
    blocks, (out, accs) = refs[:-2], refs[-2:]
    req_dev = out.shape[0]
    half = req_dev // 2
    start = HEADS * req_dev
    peaks, totals = [], []
    for block in blocks:
        stats = block[start:, :].astype(jnp.float32)
        lines = [stats[half * i : half * (i + 1)] for i in range(6)]
        peaks.append(lines[0] + lines[1] + lines[2])
        totals.append(lines[3] + lines[4] + lines[5])
    top = functools.reduce(jnp.maximum, peaks)
    shares = [total * jnp.exp(peak - top) for peak, total in zip(peaks, totals)]
    whole = functools.reduce(jnp.add, shares)
    lane = lax.broadcasted_iota(jnp.int32, whole.shape, 1)
    whole = jnp.where(lane % HALF < HEADS, whole, 1.0)
    weights = [share / whole for share in shares]
    used = half * len(blocks)
    pad = jnp.zeros((LANES - used, LANES), jnp.float32)
    turned = jnp.transpose(jnp.concatenate(weights + [pad], axis=0))
    for r in range(req_dev):
        base = HALF * (r // half)
        acc = jnp.zeros((HEADS, HEAD_DIM), jnp.float32)
        for b, block in enumerate(blocks):
            column = half * b + r % half
            weight = turned[base : base + HEADS, column : column + 1]
            acc = acc + block[HEADS * r : HEADS * (r + 1), :].astype(jnp.float32) * weight
        accs[HEADS * r : HEADS * (r + 1), :] = acc
    for h in range(HEADS):
        out[:, LANES * h : LANES * (h + 1)] = accs[pl.ds(h, req_dev, stride=HEADS), :].astype(out.dtype)


def home_merge(blocks, req_dev):
    vmem = pl.BlockSpec(memory_space=pltpu.VMEM)
    return pl.pallas_call(
        home_kernel,
        name="home_merge",
        out_shape=jax.ShapeDtypeStruct((req_dev, HEADS * HEAD_DIM), jnp.bfloat16),
        in_specs=[vmem] * len(blocks),
        out_specs=vmem,
        scratch_shapes=[pltpu.VMEM((req_dev * HEADS, HEAD_DIM), jnp.float32)],
        compiler_params=pltpu.CompilerParams(vmem_limit_bytes=16 * 2**20),
    )(*blocks)


def body(queries, keys, values, page_request, page_fill):
    count = lax.axis_size("seq")
    req_dev = queries.shape[0]
    by_xor = count <= 16
    if by_xor:
        pieces = gather_queries(queries, count)
        pieces[count // 2] = pass_on(pieces[count // 2])
    else:
        pieces = [lax.all_gather(queries, "seq", axis=0)]
    own = attend(pieces, by_xor, count, keys, values, page_request, page_fill, req_dev)
    _, given = lax.optimization_barrier((own, page_request))
    requests = [page_request] + [exchange(given, k, count) for k in range(1, LAYER)]
    across = exchange(own, 2, count)
    rows = [own, exchange(own, 1, count), across, exchange(across, 1, count)]
    blocks = list(layer_merge(requests, rows, count // LAYER, req_dev))
    for k in range(count // LAYER - 1, 0, -1):
        blocks[k] = exchange(blocks[k], LAYER * k, count)
    return home_merge(blocks, req_dev)


def solution(mesh):
    placed = (
        P(("cell", "seq"), None),
        P(("cell", "seq"), None, None),
        P(("cell", "seq"), None, None),
        P(("cell", "seq")),
        P(("cell", "seq")),
    )
    return jax.shard_map(
        body, mesh=mesh, in_specs=placed, out_specs=P(("cell", "seq"), None), check_vma=False
    )
```

```python
import functools

import jax
import jax.numpy as jnp
from jax import lax
from jax.experimental import pallas as pl
from jax.experimental.pallas import tpu as pltpu
from jax.sharding import PartitionSpec as P

HEADS = 48
KV_HEADS = 8
HEAD_DIM = 128
GROUP = 6
LANES = 128
HALF = LANES // 2

FLOOR = -30000.0
LAYER = 4
PASS_FLOPS = 20_000_000_000


def exchange(x, step, count):
    return lax.ppermute(x, "seq", [(i, i ^ step) for i in range(count)])


def gather_queries(queries, count):
    far = [4 * k for k in range(count // 4 - 1, 0, -1)]
    pieces = {0: queries}
    for step in far:
        pieces[step] = exchange(queries, step, count)
    for step in [0] + far[::-1]:
        pieces[step ^ 2] = exchange(pieces[step], 2, count)
    for step in list(pieces):
        pieces[step ^ 1] = exchange(pieces[step], 1, count)
    return [pieces[k] for k in range(count)]


def pass_kernel(source, target):
    del source, target


def pass_on(x):
    spec = pl.BlockSpec(memory_space=pltpu.VMEM)
    return pl.pallas_call(
        pass_kernel,
        name="pass_on",
        out_shape=jax.ShapeDtypeStruct(x.shape, x.dtype),
        in_specs=[spec],
        out_specs=spec,
        input_output_aliases={0: 0},
        compiler_params=pltpu.CompilerParams(vmem_limit_bytes=16 * 2**20),
        cost_estimate=pl.CostEstimate(flops=PASS_FLOPS, bytes_accessed=0, transcendentals=0),
    )(x)


def split3(x):
    high = x.astype(jnp.bfloat16).astype(jnp.float32)
    middle = (x - high).astype(jnp.bfloat16).astype(jnp.float32)
    low = (x - high - middle).astype(jnp.bfloat16).astype(jnp.float32)
    return [high, middle, low]


def attend_kernel(blocks, by_xor, request, fill, *refs):
    query_refs, (keys, values, send, held, spread, accs) = refs[:blocks], refs[blocks:]
    pages, page_len, _ = keys.shape
    homes, req_dev, width = held.shape
    me = lax.axis_index("seq") if by_xor else 0
    if by_xor:
        for k in range(blocks):
            held[k] = query_refs[k][...]
    else:
        held[...] = query_refs[0][...]
    lane = lax.broadcasted_iota(jnp.int32, (HEADS, LANES), 1)
    kv_of = lax.broadcasted_iota(jnp.int32, (HEADS, LANES), 0) // GROUP

    for p in range(pages):
        block = held[(request[p] // req_dev) ^ me].astype(jnp.float32)
        for h in range(HEADS):
            spread[p, req_dev * h : req_dev * (h + 1), :] = block[:, LANES * h : LANES * (h + 1)]
        query = spread[p, pl.ds(request[p] % req_dev, HEADS, stride=req_dev), :].astype(jnp.bfloat16)
        zero = jnp.zeros_like(query)
        wide = jnp.concatenate([jnp.where(kv_of == k, query, zero) for k in range(KV_HEADS)], axis=1)
        accs[p] = lax.dot_general(
            wide, keys[p], (((1,), (1,)), ((), ())), preferred_element_type=jnp.float32
        ) * HEAD_DIM ** (-0.5)

    heavy, totals = [], []
    stats = jnp.zeros((HEADS, LANES), jnp.float32)
    for p in range(pages):
        scores = accs[p]
        live = lax.broadcasted_iota(jnp.int32, (HEADS, page_len), 1) < fill[p]
        peak = jnp.max(jnp.where(live, scores, FLOOR), axis=1, keepdims=True)
        weights = jnp.where(live, jnp.exp(scores - peak), 0.0).astype(jnp.bfloat16)
        total = jnp.sum(weights.astype(jnp.float32), axis=1, keepdims=True)
        heavy.append(weights)
        totals.append(total)
        stats = jnp.where(lane == p, peak, stats)
        stats = jnp.where(lane == pages + p, total, stats)
    high, middle, low = split3(stats)
    stats = high + pltpu.roll(middle, 2 * pages, 1) + pltpu.roll(low, 4 * pages, 1)
    send[HEADS * pages :, :] = stats.astype(send.dtype)

    for p in range(pages):
        mixed = lax.dot_general(
            heavy[p], values[p], (((1,), (0,)), ((), ())), preferred_element_type=jnp.float32
        )
        acc = mixed[:, :LANES]
        for k in range(1, KV_HEADS):
            acc = jnp.where(kv_of == k, mixed[:, LANES * k : LANES * (k + 1)], acc)
        send[HEADS * p : HEADS * (p + 1), :] = (acc / jnp.maximum(totals[p], 1.0)).astype(send.dtype)


def attend(pieces, by_xor, count, keys, values, page_request, page_fill, req_dev):
    pages = keys.shape[0]
    width = HEADS * HEAD_DIM
    vmem = pl.BlockSpec(memory_space=pltpu.VMEM)
    smem = pl.BlockSpec(memory_space=pltpu.SMEM)
    return pl.pallas_call(
        functools.partial(attend_kernel, len(pieces), by_xor),
        name="attend",
        out_shape=jax.ShapeDtypeStruct(((pages + 1) * HEADS, LANES), jnp.bfloat16),
        in_specs=[smem, smem] + [vmem] * (len(pieces) + 2),
        out_specs=vmem,
        scratch_shapes=[
            pltpu.VMEM((count, req_dev, width), jnp.bfloat16),
            pltpu.VMEM((pages, HEADS * req_dev, LANES), jnp.float32),
            pltpu.VMEM((pages, HEADS, HEAD_DIM), jnp.float32),
        ],
        compiler_params=pltpu.CompilerParams(vmem_limit_bytes=32 * 2**20),
    )(page_request, page_fill, *pieces, keys, values)


def layer_kernel(req_dev, *refs):
    requests, rows, outs, sums = refs[:LAYER], refs[LAYER : 2 * LAYER], refs[2 * LAYER : -1], refs[-1]
    pages = rows[0].shape[0] // HEADS - 1
    homes = len(outs)
    slots = homes * req_dev
    me = lax.axis_index("seq")
    lane = lax.broadcasted_iota(jnp.int32, (HEADS, LANES), 1)
    sums[...] = jnp.zeros_like(sums)

    place, peaks, totals = [], jnp.full((HEADS, LANES), FLOOR, jnp.float32), jnp.zeros((HEADS, LANES), jnp.float32)
    where = jnp.full((1, LANES), -1, jnp.int32)
    for s in range(LAYER):
        stats = rows[s][HEADS * pages :, :].astype(jnp.float32)
        stats = stats + pltpu.roll(stats, LANES - 2 * pages, 1) + pltpu.roll(stats, LANES - 4 * pages, 1)
        inside = jnp.logical_and(lane >= pages * s, lane < pages * (s + 1))
        peaks = jnp.where(inside, pltpu.roll(stats, (pages * s) % LANES, 1), peaks)
        totals = jnp.where(inside, pltpu.roll(stats, (pages * (s - 1)) % LANES, 1), totals)
        for p in range(pages):
            apart = (requests[s][p] // req_dev) ^ me
            mine = apart % LAYER == 0
            place.append(jnp.where(mine, apart // LAYER * req_dev + requests[s][p] % req_dev, slots))
            where = jnp.where(lane[:1] == len(place) - 1, place[-1], where)

    masks = [where == k for k in range(slots)]
    tops = jnp.zeros((HEADS, LANES), jnp.float32)
    slot_tops = jnp.full((HEADS, LANES), FLOOR, jnp.float32)
    for k in range(slots):
        top = jnp.max(jnp.where(masks[k], peaks, FLOOR), axis=1, keepdims=True)
        tops = jnp.where(masks[k], top, tops)
        slot_tops = jnp.where(lane == k, top, slot_tops)
    shares = jnp.where(where < slots, totals * jnp.exp(peaks - tops), 0.0)
    wholes = []
    slot_wholes = jnp.zeros((HEADS, LANES), jnp.float32)
    for k in range(slots):
        whole = jnp.sum(jnp.where(masks[k], shares, 0.0), axis=1, keepdims=True)
        slot_wholes = jnp.where(lane == k, whole, slot_wholes)
        wholes.append(jnp.maximum(whole, 1.0))
    for i, at in enumerate(place):
        s, p = divmod(i, pages)
        sums[at] += rows[s][HEADS * p : HEADS * (p + 1), :].astype(jnp.float32) * shares[:, i : i + 1]

    pad = jnp.zeros((LANES - HEADS, LANES), jnp.float32)
    parts = []
    for table in (slot_tops, slot_wholes):
        flat = jnp.transpose(jnp.concatenate([table, pad], axis=0))
        parts += split3(flat[:slots])
    for k in range(homes):
        for r in range(req_dev):
            slot = req_dev * k + r
            outs[k][HEADS * r : HEADS * (r + 1), :] = (sums[slot] / wholes[slot]).astype(outs[k].dtype)
        lines = []
        for part in parts:
            block = part[req_dev * k : req_dev * (k + 1)]
            block = jnp.concatenate([block, jnp.zeros((8 - req_dev, LANES), jnp.float32)], axis=0)
            lines.append(block + pltpu.roll(pltpu.roll(block, 8 - req_dev // 2, 0), HALF, 1))
        tail = [line[: req_dev // 2] for line in lines]
        spare = outs[k].shape[0] - HEADS * req_dev - 3 * req_dev
        if spare:
            tail.append(jnp.zeros((spare, LANES), jnp.float32))
        outs[k][HEADS * req_dev :, :] = jnp.concatenate(tail, axis=0).astype(outs[k].dtype)


def layer_merge(requests, rows, homes, req_dev):
    vmem = pl.BlockSpec(memory_space=pltpu.VMEM)
    smem = pl.BlockSpec(memory_space=pltpu.SMEM)
    height = HEADS * req_dev + -(-3 * req_dev // 8) * 8
    return pl.pallas_call(
        functools.partial(layer_kernel, req_dev),
        name="layer_merge",
        out_shape=[jax.ShapeDtypeStruct((height, LANES), jnp.bfloat16)] * homes,
        in_specs=[smem] * LAYER + [vmem] * LAYER,
        out_specs=[vmem] * homes,
        scratch_shapes=[pltpu.VMEM((homes * req_dev + 1, HEADS, HEAD_DIM), jnp.float32)],
        compiler_params=pltpu.CompilerParams(vmem_limit_bytes=16 * 2**20),
    )(*requests, *rows)


def home_kernel(*refs):
    blocks, (out, accs) = refs[:-2], refs[-2:]
    req_dev = out.shape[0]
    half = req_dev // 2
    start = HEADS * req_dev
    peaks, totals = [], []
    for block in blocks:
        stats = block[start:, :].astype(jnp.float32)
        lines = [stats[half * i : half * (i + 1)] for i in range(6)]
        peaks.append(lines[0] + lines[1] + lines[2])
        totals.append(lines[3] + lines[4] + lines[5])
    top = functools.reduce(jnp.maximum, peaks)
    shares = [total * jnp.exp(peak - top) for peak, total in zip(peaks, totals)]
    whole = functools.reduce(jnp.add, shares)
    lane = lax.broadcasted_iota(jnp.int32, whole.shape, 1)
    whole = jnp.where(lane % HALF < HEADS, whole, 1.0)
    weights = [share / whole for share in shares]
    used = half * len(blocks)
    pad = jnp.zeros((LANES - used, LANES), jnp.float32)
    turned = jnp.transpose(jnp.concatenate(weights + [pad], axis=0))
    for r in range(req_dev):
        base = HALF * (r // half)
        acc = jnp.zeros((HEADS, HEAD_DIM), jnp.float32)
        for b, block in enumerate(blocks):
            column = half * b + r % half
            weight = turned[base : base + HEADS, column : column + 1]
            acc = acc + block[HEADS * r : HEADS * (r + 1), :].astype(jnp.float32) * weight
        accs[HEADS * r : HEADS * (r + 1), :] = acc
    for h in range(HEADS):
        out[:, LANES * h : LANES * (h + 1)] = accs[pl.ds(h, req_dev, stride=HEADS), :].astype(out.dtype)


def home_merge(blocks, req_dev):
    vmem = pl.BlockSpec(memory_space=pltpu.VMEM)
    return pl.pallas_call(
        home_kernel,
        name="home_merge",
        out_shape=jax.ShapeDtypeStruct((req_dev, HEADS * HEAD_DIM), jnp.bfloat16),
        in_specs=[vmem] * len(blocks),
        out_specs=vmem,
        scratch_shapes=[pltpu.VMEM((req_dev * HEADS, HEAD_DIM), jnp.float32)],
        compiler_params=pltpu.CompilerParams(vmem_limit_bytes=16 * 2**20),
    )(*blocks)


def body(queries, keys, values, page_request, page_fill):
    count = lax.axis_size("seq")
    req_dev = queries.shape[0]
    by_xor = count <= 16
    if by_xor:
        pieces = gather_queries(queries, count)
        pieces[count // 2] = pass_on(pieces[count // 2])
    else:
        pieces = [lax.all_gather(queries, "seq", axis=0)]
    own = attend(pieces, by_xor, count, keys, values, page_request, page_fill, req_dev)
    _, given = lax.optimization_barrier((own, page_request))
    requests = [page_request] + [exchange(given, k, count) for k in range(1, LAYER)]
    across = exchange(own, 2, count)
    beside = exchange(own, 1, count)
    across, *requests = lax.optimization_barrier((across, *requests))
    rows = [own, beside, across, exchange(across, 1, count)]
    blocks = list(layer_merge(requests, rows, count // LAYER, req_dev))
    far = [exchange(blocks[k], LAYER * k, count) for k in range(count // LAYER - 1, 0, -1)]
    return home_merge(blocks[:1] + far, req_dev)


def solution(mesh):
    placed = (
        P(("cell", "seq"), None),
        P(("cell", "seq"), None, None),
        P(("cell", "seq"), None, None),
        P(("cell", "seq")),
        P(("cell", "seq")),
    )
    return jax.shard_map(
        body, mesh=mesh, in_specs=placed, out_specs=P(("cell", "seq"), None), check_vma=False
    )
```

```python
import functools

import jax
import jax.numpy as jnp
from jax import lax
from jax.experimental import pallas as pl
from jax.experimental.pallas import tpu as pltpu
from jax.sharding import PartitionSpec as P

HEADS = 48
KV_HEADS = 8
HEAD_DIM = 128
GROUP = 6
LANES = 128
HALF = LANES // 2

FLOOR = -30000.0
LAYER = 4
PASS_FLOPS = 20_000_000_000


def exchange(x, step, count):
    return lax.ppermute(x, "seq", [(i, i ^ step) for i in range(count)])


def gather_queries(queries, count):
    far = [4 * k for k in range(count // 4 - 1, 0, -1)]
    pieces = {0: queries}
    for step in far:
        pieces[step] = exchange(queries, step, count)
    for step in [0] + far[::-1]:
        pieces[step ^ 2] = exchange(pieces[step], 2, count)
    for step in list(pieces):
        pieces[step ^ 1] = exchange(pieces[step], 1, count)
    return [pieces[k] for k in range(count)]


def pass_kernel(source, target):
    del source, target


def pass_on(x):
    spec = pl.BlockSpec(memory_space=pltpu.VMEM)
    return pl.pallas_call(
        pass_kernel,
        name="pass_on",
        out_shape=jax.ShapeDtypeStruct(x.shape, x.dtype),
        in_specs=[spec],
        out_specs=spec,
        input_output_aliases={0: 0},
        compiler_params=pltpu.CompilerParams(vmem_limit_bytes=16 * 2**20),
        cost_estimate=pl.CostEstimate(flops=PASS_FLOPS, bytes_accessed=0, transcendentals=0),
    )(x)


def split3(x):
    high = x.astype(jnp.bfloat16).astype(jnp.float32)
    middle = (x - high).astype(jnp.bfloat16).astype(jnp.float32)
    low = (x - high - middle).astype(jnp.bfloat16).astype(jnp.float32)
    return [high, middle, low]


def scalars(x):
    return [x[0, i] for i in range(x.shape[1])]


def divide(x, by):
    return x >> by.bit_length() - 1 if by & (by - 1) == 0 else x // by


def remainder(x, by):
    return x & (by - 1) if by & (by - 1) == 0 else x % by


def attend_kernel(blocks, by_xor, request_ref, fill_ref, *refs):
    query_refs, (keys, values, send, held, spread, accs) = refs[:blocks], refs[blocks:]
    pages, page_len, _ = keys.shape
    homes, req_dev, width = held.shape
    me = lax.axis_index("seq") if by_xor else 0
    where = request_ref[...]
    block_at = scalars(divide(where, req_dev) ^ me)
    row_at = scalars(remainder(where, req_dev))
    fill = scalars(fill_ref[...])
    if by_xor:
        for k in range(blocks):
            held[k] = query_refs[k][...]
    else:
        held[...] = query_refs[0][...]
    lane = lax.broadcasted_iota(jnp.int32, (HEADS, LANES), 1)
    kv_of = lax.broadcasted_iota(jnp.int32, (HEADS, LANES), 0) // GROUP

    for p in range(pages):
        block = held[block_at[p]].astype(jnp.float32)
        for h in range(HEADS):
            spread[p, req_dev * h : req_dev * (h + 1), :] = block[:, LANES * h : LANES * (h + 1)]
        query = spread[p, pl.ds(row_at[p], HEADS, stride=req_dev), :].astype(jnp.bfloat16)
        zero = jnp.zeros_like(query)
        wide = jnp.concatenate([jnp.where(kv_of == k, query, zero) for k in range(KV_HEADS)], axis=1)
        accs[p] = lax.dot_general(
            wide, keys[p], (((1,), (1,)), ((), ())), preferred_element_type=jnp.float32
        ) * HEAD_DIM ** (-0.5)

    heavy, totals = [], []
    stats = jnp.zeros((HEADS, LANES), jnp.float32)
    for p in range(pages):
        scores = accs[p]
        live = lax.broadcasted_iota(jnp.int32, (HEADS, page_len), 1) < fill[p]
        peak = jnp.max(jnp.where(live, scores, FLOOR), axis=1, keepdims=True)
        weights = jnp.where(live, jnp.exp(scores - peak), 0.0).astype(jnp.bfloat16)
        total = jnp.sum(weights.astype(jnp.float32), axis=1, keepdims=True)
        heavy.append(weights)
        totals.append(total)
        stats = jnp.where(lane == p, peak, stats)
        stats = jnp.where(lane == pages + p, total, stats)
    high, middle, low = split3(stats)
    stats = high + pltpu.roll(middle, 2 * pages, 1) + pltpu.roll(low, 4 * pages, 1)
    send[HEADS * pages :, :] = stats.astype(send.dtype)

    for p in range(pages):
        mixed = lax.dot_general(
            heavy[p], values[p], (((1,), (0,)), ((), ())), preferred_element_type=jnp.float32
        )
        acc = mixed[:, :LANES]
        for k in range(1, KV_HEADS):
            acc = jnp.where(kv_of == k, mixed[:, LANES * k : LANES * (k + 1)], acc)
        send[HEADS * p : HEADS * (p + 1), :] = (acc / jnp.maximum(totals[p], 1.0)).astype(send.dtype)


def attend(pieces, by_xor, count, keys, values, page_request, page_fill, req_dev):
    pages = keys.shape[0]
    width = HEADS * HEAD_DIM
    vmem = pl.BlockSpec(memory_space=pltpu.VMEM)
    return pl.pallas_call(
        functools.partial(attend_kernel, len(pieces), by_xor),
        name="attend",
        out_shape=jax.ShapeDtypeStruct(((pages + 1) * HEADS, LANES), jnp.bfloat16),
        in_specs=[vmem] * (len(pieces) + 4),
        out_specs=vmem,
        scratch_shapes=[
            pltpu.VMEM((count, req_dev, width), jnp.bfloat16),
            pltpu.VMEM((pages, HEADS * req_dev, LANES), jnp.float32),
            pltpu.VMEM((pages, HEADS, HEAD_DIM), jnp.float32),
        ],
        compiler_params=pltpu.CompilerParams(vmem_limit_bytes=32 * 2**20),
    )(page_request, page_fill, *pieces, keys, values)


def layer_kernel(req_dev, *refs):
    requests, rows, outs, sums = refs[:LAYER], refs[LAYER : 2 * LAYER], refs[2 * LAYER : -1], refs[-1]
    pages = rows[0].shape[0] // HEADS - 1
    homes = len(outs)
    slots = homes * req_dev
    me = lax.axis_index("seq")
    lane = lax.broadcasted_iota(jnp.int32, (HEADS, LANES), 1)
    sums[...] = jnp.zeros_like(sums)

    spare = jnp.full((1, LANES - LAYER * pages), -1, jnp.int32)
    request = jnp.concatenate([r[...] for r in requests] + [spare], axis=1)
    apart = divide(request, req_dev) ^ me
    mine = jnp.logical_and(request >= 0, remainder(apart, LAYER) == 0)
    where = jnp.where(mine, divide(apart, LAYER) * req_dev + remainder(request, req_dev), slots)
    place = scalars(where[:, : LAYER * pages])

    peaks, totals = jnp.full((HEADS, LANES), FLOOR, jnp.float32), jnp.zeros((HEADS, LANES), jnp.float32)
    for s in range(LAYER):
        stats = rows[s][HEADS * pages :, :].astype(jnp.float32)
        stats = stats + pltpu.roll(stats, LANES - 2 * pages, 1) + pltpu.roll(stats, LANES - 4 * pages, 1)
        inside = jnp.logical_and(lane >= pages * s, lane < pages * (s + 1))
        peaks = jnp.where(inside, pltpu.roll(stats, (pages * s) % LANES, 1), peaks)
        totals = jnp.where(inside, pltpu.roll(stats, (pages * (s - 1)) % LANES, 1), totals)

    masks = [where == k for k in range(slots)]
    tops = jnp.zeros((HEADS, LANES), jnp.float32)
    slot_tops = jnp.full((HEADS, LANES), FLOOR, jnp.float32)
    for k in range(slots):
        top = jnp.max(jnp.where(masks[k], peaks, FLOOR), axis=1, keepdims=True)
        tops = jnp.where(masks[k], top, tops)
        slot_tops = jnp.where(lane == k, top, slot_tops)
    shares = jnp.where(where < slots, totals * jnp.exp(peaks - tops), 0.0)
    norms = jnp.ones((HEADS, LANES), jnp.float32)
    slot_wholes = jnp.zeros((HEADS, LANES), jnp.float32)
    for k in range(slots):
        whole = jnp.sum(jnp.where(masks[k], shares, 0.0), axis=1, keepdims=True)
        slot_wholes = jnp.where(lane == k, whole, slot_wholes)
        norms = jnp.where(masks[k], whole, norms)
    shares = shares / jnp.maximum(norms, 1.0)
    for i, at in enumerate(place):
        s, p = divmod(i, pages)
        sums[at] += rows[s][HEADS * p : HEADS * (p + 1), :].astype(jnp.float32) * shares[:, i : i + 1]

    pad = jnp.zeros((LANES - HEADS, LANES), jnp.float32)
    parts = []
    for table in (slot_tops, slot_wholes):
        flat = jnp.transpose(jnp.concatenate([table, pad], axis=0))
        parts += split3(flat[:slots])
    for k in range(homes):
        for r in range(req_dev):
            outs[k][HEADS * r : HEADS * (r + 1), :] = sums[req_dev * k + r].astype(outs[k].dtype)
        lines = []
        for part in parts:
            block = part[req_dev * k : req_dev * (k + 1)]
            block = jnp.concatenate([block, jnp.zeros((8 - req_dev, LANES), jnp.float32)], axis=0)
            lines.append(block + pltpu.roll(pltpu.roll(block, 8 - req_dev // 2, 0), HALF, 1))
        tail = [line[: req_dev // 2] for line in lines]
        spare = outs[k].shape[0] - HEADS * req_dev - 3 * req_dev
        if spare:
            tail.append(jnp.zeros((spare, LANES), jnp.float32))
        outs[k][HEADS * req_dev :, :] = jnp.concatenate(tail, axis=0).astype(outs[k].dtype)


def layer_merge(requests, rows, homes, req_dev):
    vmem = pl.BlockSpec(memory_space=pltpu.VMEM)
    height = HEADS * req_dev + -(-3 * req_dev // 8) * 8
    return pl.pallas_call(
        functools.partial(layer_kernel, req_dev),
        name="layer_merge",
        out_shape=[jax.ShapeDtypeStruct((height, LANES), jnp.bfloat16)] * homes,
        in_specs=[vmem] * (2 * LAYER),
        out_specs=[vmem] * homes,
        scratch_shapes=[pltpu.VMEM((homes * req_dev + 1, HEADS, HEAD_DIM), jnp.float32)],
        compiler_params=pltpu.CompilerParams(vmem_limit_bytes=16 * 2**20),
    )(*requests, *rows)


def home_kernel(*refs):
    blocks, (out, accs) = refs[:-2], refs[-2:]
    req_dev = out.shape[0]
    half = req_dev // 2
    start = HEADS * req_dev
    peaks, totals = [], []
    for block in blocks:
        stats = block[start:, :].astype(jnp.float32)
        lines = [stats[half * i : half * (i + 1)] for i in range(6)]
        peaks.append(lines[0] + lines[1] + lines[2])
        totals.append(lines[3] + lines[4] + lines[5])
    top = functools.reduce(jnp.maximum, peaks)
    shares = [total * jnp.exp(peak - top) for peak, total in zip(peaks, totals)]
    whole = functools.reduce(jnp.add, shares)
    lane = lax.broadcasted_iota(jnp.int32, whole.shape, 1)
    whole = jnp.where(lane % HALF < HEADS, whole, 1.0)
    weights = [share / whole for share in shares]
    used = half * len(blocks)
    pad = jnp.zeros((LANES - used, LANES), jnp.float32)
    turned = jnp.transpose(jnp.concatenate(weights + [pad], axis=0))
    for r in range(req_dev):
        base = HALF * (r // half)
        acc = jnp.zeros((HEADS, HEAD_DIM), jnp.float32)
        for b, block in enumerate(blocks):
            column = half * b + r % half
            weight = turned[base : base + HEADS, column : column + 1]
            acc = acc + block[HEADS * r : HEADS * (r + 1), :].astype(jnp.float32) * weight
        accs[HEADS * r : HEADS * (r + 1), :] = acc
    for h in range(HEADS):
        out[:, LANES * h : LANES * (h + 1)] = accs[pl.ds(h, req_dev, stride=HEADS), :].astype(out.dtype)


def home_merge(blocks, req_dev):
    vmem = pl.BlockSpec(memory_space=pltpu.VMEM)
    return pl.pallas_call(
        home_kernel,
        name="home_merge",
        out_shape=jax.ShapeDtypeStruct((req_dev, HEADS * HEAD_DIM), jnp.bfloat16),
        in_specs=[vmem] * len(blocks),
        out_specs=vmem,
        scratch_shapes=[pltpu.VMEM((req_dev * HEADS, HEAD_DIM), jnp.float32)],
        compiler_params=pltpu.CompilerParams(vmem_limit_bytes=16 * 2**20),
    )(*blocks)


def body(queries, keys, values, page_request, page_fill):
    count = lax.axis_size("seq")
    req_dev = queries.shape[0]
    page_request, page_fill = page_request[None], page_fill[None]
    by_xor = count <= 16
    if by_xor:
        pieces = gather_queries(queries, count)
        pieces[count // 2] = pass_on(pieces[count // 2])
    else:
        pieces = [lax.all_gather(queries, "seq", axis=0)]
    own = attend(pieces, by_xor, count, keys, values, page_request, page_fill, req_dev)
    _, given = lax.optimization_barrier((own, page_request))
    requests = [page_request] + [exchange(given, k, count) for k in range(1, LAYER)]
    across = exchange(own, 2, count)
    beside = exchange(own, 1, count)
    across, *requests = lax.optimization_barrier((across, *requests))
    rows = [own, beside, across, exchange(across, 1, count)]
    blocks = list(layer_merge(requests, rows, count // LAYER, req_dev))
    far = [exchange(blocks[k], LAYER * k, count) for k in range(count // LAYER - 1, 0, -1)]
    return home_merge(blocks[:1] + far, req_dev)


def solution(mesh):
    placed = (
        P(("cell", "seq"), None),
        P(("cell", "seq"), None, None),
        P(("cell", "seq"), None, None),
        P(("cell", "seq")),
        P(("cell", "seq")),
    )
    return jax.shard_map(
        body, mesh=mesh, in_specs=placed, out_specs=P(("cell", "seq"), None), check_vma=False
    )
```

```python
import functools

import jax
import jax.numpy as jnp
from jax import lax
from jax.experimental import pallas as pl
from jax.experimental.pallas import tpu as pltpu
from jax.sharding import PartitionSpec as P

HEADS = 48
KV_HEADS = 8
HEAD_DIM = 128
GROUP = 6
LANES = 128
HALF = LANES // 2

FLOOR = -30000.0
LAYER = 4
STAGE_FLOPS = 20_000_000_000


def exchange(x, step, count):
    return lax.ppermute(x, "seq", [(i, i ^ step) for i in range(count)])


def gather_queries(queries, count):
    far = [4 * k for k in range(count // 4 - 1, 0, -1)]
    pieces = {0: queries}
    for step in far:
        pieces[step] = exchange(queries, step, count)
    for step in [0] + far[::-1]:
        pieces[step ^ 2] = exchange(pieces[step], 2, count)
    for step in list(pieces):
        pieces[step ^ 1] = exchange(pieces[step], 1, count)
    return [pieces[k] for k in range(count)]


def spread_out(block, rows, put):
    req_dev = block.shape[0]
    block = block[...].astype(jnp.float32)
    for h in range(HEADS):
        rows[req_dev * h : req_dev * (h + 1), :] = block[:, LANES * h : LANES * (h + 1)]
    for r in range(req_dev):
        put(r, rows[pl.ds(r, HEADS, stride=req_dev), :].astype(jnp.bfloat16))


def stage_kernel(*refs):
    blocks, (held, rows) = refs[:-2], refs[-2:]
    for k, block in enumerate(blocks):

        def put(r, tile, k=k):
            held[k, r] = tile

        spread_out(block, rows.at[k], put)


def stage(blocks):
    spec = pl.BlockSpec(memory_space=pltpu.VMEM)
    req_dev = blocks[0].shape[0]
    return pl.pallas_call(
        stage_kernel,
        name="stage",
        out_shape=jax.ShapeDtypeStruct((len(blocks), req_dev, HEADS, HEAD_DIM), jnp.bfloat16),
        in_specs=[spec] * len(blocks),
        out_specs=spec,
        scratch_shapes=[pltpu.VMEM((len(blocks), HEADS * req_dev, LANES), jnp.float32)],
        compiler_params=pltpu.CompilerParams(vmem_limit_bytes=16 * 2**20),
        cost_estimate=pl.CostEstimate(flops=STAGE_FLOPS, bytes_accessed=0, transcendentals=0),
    )(*blocks)


def split3(x):
    high = x.astype(jnp.bfloat16).astype(jnp.float32)
    middle = (x - high).astype(jnp.bfloat16).astype(jnp.float32)
    low = (x - high - middle).astype(jnp.bfloat16).astype(jnp.float32)
    return [high, middle, low]


def scalars(x):
    return [x[0, i] for i in range(x.shape[1])]


def divide(x, by):
    return x >> by.bit_length() - 1 if by & (by - 1) == 0 else x // by


def remainder(x, by):
    return x & (by - 1) if by & (by - 1) == 0 else x % by


def attend_kernel(late, by_xor, request_ref, fill_ref, held, *refs):
    late_refs, (keys, values, send, tail, rows, accs) = refs[:late], refs[late:]
    pages, page_len, _ = keys.shape
    early, req_dev, _, _ = held.shape
    me = lax.axis_index("seq") if by_xor else 0
    where = request_ref[...]
    block_at = divide(where, req_dev)
    if by_xor:
        block_at = remainder((block_at ^ me) + early + late - 1, early + late)
    block_at = scalars(block_at)
    row_at = scalars(remainder(where, req_dev))
    fill = scalars(fill_ref[...])
    for k in range(late):

        def put(r, tile, k=k):
            tail[k, r] = tile

        spread_out(late_refs[k], rows.at[k], put)
    lane = lax.broadcasted_iota(jnp.int32, (HEADS, LANES), 1)
    kv_of = lax.broadcasted_iota(jnp.int32, (HEADS, LANES), 0) // GROUP

    for p in range(pages):
        query = held[jnp.minimum(block_at[p], early - 1), row_at[p]]
        if late:
            last = tail[jnp.maximum(block_at[p] - early, 0), row_at[p]]
            query = jnp.where(block_at[p] < early, query, last)
        zero = jnp.zeros_like(query)
        wide = jnp.concatenate([jnp.where(kv_of == k, query, zero) for k in range(KV_HEADS)], axis=1)
        accs[p] = lax.dot_general(
            wide, keys[p], (((1,), (1,)), ((), ())), preferred_element_type=jnp.float32
        ) * HEAD_DIM ** (-0.5)

    heavy, totals = [], []
    stats = jnp.zeros((HEADS, LANES), jnp.float32)
    for p in range(pages):
        scores = accs[p]
        live = lax.broadcasted_iota(jnp.int32, (HEADS, page_len), 1) < fill[p]
        peak = jnp.max(jnp.where(live, scores, FLOOR), axis=1, keepdims=True)
        weights = jnp.where(live, jnp.exp(scores - peak), 0.0).astype(jnp.bfloat16)
        total = jnp.sum(weights.astype(jnp.float32), axis=1, keepdims=True)
        heavy.append(weights)
        totals.append(total)
        stats = jnp.where(lane == p, peak, stats)
        stats = jnp.where(lane == pages + p, total, stats)
    high, middle, low = split3(stats)
    stats = high + pltpu.roll(middle, 2 * pages, 1) + pltpu.roll(low, 4 * pages, 1)
    send[HEADS * pages :, :] = stats.astype(send.dtype)

    for p in range(pages):
        mixed = lax.dot_general(
            heavy[p], values[p], (((1,), (0,)), ((), ())), preferred_element_type=jnp.float32
        )
        acc = mixed[:, :LANES]
        for k in range(1, KV_HEADS):
            acc = jnp.where(kv_of == k, mixed[:, LANES * k : LANES * (k + 1)], acc)
        send[HEADS * p : HEADS * (p + 1), :] = (acc / jnp.maximum(totals[p], 1.0)).astype(send.dtype)


def attend(held, late, by_xor, keys, values, page_request, page_fill):
    pages = keys.shape[0]
    req_dev = held.shape[1]
    vmem = pl.BlockSpec(memory_space=pltpu.VMEM)
    return pl.pallas_call(
        functools.partial(attend_kernel, len(late), by_xor),
        name="attend",
        out_shape=jax.ShapeDtypeStruct(((pages + 1) * HEADS, LANES), jnp.bfloat16),
        in_specs=[vmem] * (len(late) + 5),
        out_specs=vmem,
        scratch_shapes=[
            pltpu.VMEM((max(len(late), 1), req_dev, HEADS, HEAD_DIM), jnp.bfloat16),
            pltpu.VMEM((max(len(late), 1), HEADS * req_dev, LANES), jnp.float32),
            pltpu.VMEM((pages, HEADS, HEAD_DIM), jnp.float32),
        ],
        compiler_params=pltpu.CompilerParams(vmem_limit_bytes=32 * 2**20),
    )(page_request, page_fill, held, *late, keys, values)


def layer_kernel(req_dev, *refs):
    requests, rows, outs, sums = refs[:LAYER], refs[LAYER : 2 * LAYER], refs[2 * LAYER : -1], refs[-1]
    pages = rows[0].shape[0] // HEADS - 1
    homes = len(outs)
    slots = homes * req_dev
    me = lax.axis_index("seq")
    lane = lax.broadcasted_iota(jnp.int32, (HEADS, LANES), 1)
    sums[...] = jnp.zeros_like(sums)

    spare = jnp.full((1, LANES - LAYER * pages), -1, jnp.int32)
    request = jnp.concatenate([r[...] for r in requests] + [spare], axis=1)
    apart = divide(request, req_dev) ^ me
    mine = jnp.logical_and(request >= 0, remainder(apart, LAYER) == 0)
    where = jnp.where(mine, divide(apart, LAYER) * req_dev + remainder(request, req_dev), slots)
    place = scalars(where[:, : LAYER * pages])

    peaks, totals = jnp.full((HEADS, LANES), FLOOR, jnp.float32), jnp.zeros((HEADS, LANES), jnp.float32)
    for s in range(LAYER):
        stats = rows[s][HEADS * pages :, :].astype(jnp.float32)
        stats = stats + pltpu.roll(stats, LANES - 2 * pages, 1) + pltpu.roll(stats, LANES - 4 * pages, 1)
        inside = jnp.logical_and(lane >= pages * s, lane < pages * (s + 1))
        peaks = jnp.where(inside, pltpu.roll(stats, (pages * s) % LANES, 1), peaks)
        totals = jnp.where(inside, pltpu.roll(stats, (pages * (s - 1)) % LANES, 1), totals)

    masks = [where == k for k in range(slots)]
    tops = jnp.zeros((HEADS, LANES), jnp.float32)
    slot_tops = jnp.full((HEADS, LANES), FLOOR, jnp.float32)
    for k in range(slots):
        top = jnp.max(jnp.where(masks[k], peaks, FLOOR), axis=1, keepdims=True)
        tops = jnp.where(masks[k], top, tops)
        slot_tops = jnp.where(lane == k, top, slot_tops)
    shares = jnp.where(where < slots, totals * jnp.exp(peaks - tops), 0.0)
    norms = jnp.ones((HEADS, LANES), jnp.float32)
    slot_wholes = jnp.zeros((HEADS, LANES), jnp.float32)
    for k in range(slots):
        whole = jnp.sum(jnp.where(masks[k], shares, 0.0), axis=1, keepdims=True)
        slot_wholes = jnp.where(lane == k, whole, slot_wholes)
        norms = jnp.where(masks[k], whole, norms)
    shares = shares / jnp.maximum(norms, 1.0)
    for i, at in enumerate(place):
        s, p = divmod(i, pages)
        sums[at] += rows[s][HEADS * p : HEADS * (p + 1), :].astype(jnp.float32) * shares[:, i : i + 1]

    pad = jnp.zeros((LANES - HEADS, LANES), jnp.float32)
    parts = []
    for table in (slot_tops, slot_wholes):
        flat = jnp.transpose(jnp.concatenate([table, pad], axis=0))
        parts += split3(flat[:slots])
    for k in range(homes):
        for r in range(req_dev):
            outs[k][HEADS * r : HEADS * (r + 1), :] = sums[req_dev * k + r].astype(outs[k].dtype)
        lines = []
        for part in parts:
            block = part[req_dev * k : req_dev * (k + 1)]
            block = jnp.concatenate([block, jnp.zeros((8 - req_dev, LANES), jnp.float32)], axis=0)
            lines.append(block + pltpu.roll(pltpu.roll(block, 8 - req_dev // 2, 0), HALF, 1))
        tail = [line[: req_dev // 2] for line in lines]
        spare = outs[k].shape[0] - HEADS * req_dev - 3 * req_dev
        if spare:
            tail.append(jnp.zeros((spare, LANES), jnp.float32))
        outs[k][HEADS * req_dev :, :] = jnp.concatenate(tail, axis=0).astype(outs[k].dtype)


def layer_merge(requests, rows, homes, req_dev):
    vmem = pl.BlockSpec(memory_space=pltpu.VMEM)
    height = HEADS * req_dev + -(-3 * req_dev // 8) * 8
    return pl.pallas_call(
        functools.partial(layer_kernel, req_dev),
        name="layer_merge",
        out_shape=[jax.ShapeDtypeStruct((height, LANES), jnp.bfloat16)] * homes,
        in_specs=[vmem] * (2 * LAYER),
        out_specs=[vmem] * homes,
        scratch_shapes=[pltpu.VMEM((homes * req_dev + 1, HEADS, HEAD_DIM), jnp.float32)],
        compiler_params=pltpu.CompilerParams(vmem_limit_bytes=16 * 2**20),
    )(*requests, *rows)


def home_kernel(*refs):
    blocks, (out, accs) = refs[:-2], refs[-2:]
    req_dev = out.shape[0]
    half = req_dev // 2
    start = HEADS * req_dev
    peaks, totals = [], []
    for block in blocks:
        stats = block[start:, :].astype(jnp.float32)
        lines = [stats[half * i : half * (i + 1)] for i in range(6)]
        peaks.append(lines[0] + lines[1] + lines[2])
        totals.append(lines[3] + lines[4] + lines[5])
    top = functools.reduce(jnp.maximum, peaks)
    shares = [total * jnp.exp(peak - top) for peak, total in zip(peaks, totals)]
    whole = functools.reduce(jnp.add, shares)
    lane = lax.broadcasted_iota(jnp.int32, whole.shape, 1)
    whole = jnp.where(lane % HALF < HEADS, whole, 1.0)
    weights = [share / whole for share in shares]
    used = half * len(blocks)
    pad = jnp.zeros((LANES - used, LANES), jnp.float32)
    turned = jnp.transpose(jnp.concatenate(weights + [pad], axis=0))
    for r in range(req_dev):
        base = HALF * (r // half)
        acc = jnp.zeros((HEADS, HEAD_DIM), jnp.float32)
        for b, block in enumerate(blocks):
            column = half * b + r % half
            weight = turned[base : base + HEADS, column : column + 1]
            acc = acc + block[HEADS * r : HEADS * (r + 1), :].astype(jnp.float32) * weight
        accs[HEADS * r : HEADS * (r + 1), :] = acc
    for h in range(HEADS):
        out[:, LANES * h : LANES * (h + 1)] = accs[pl.ds(h, req_dev, stride=HEADS), :].astype(out.dtype)


def home_merge(blocks, req_dev):
    vmem = pl.BlockSpec(memory_space=pltpu.VMEM)
    return pl.pallas_call(
        home_kernel,
        name="home_merge",
        out_shape=jax.ShapeDtypeStruct((req_dev, HEADS * HEAD_DIM), jnp.bfloat16),
        in_specs=[vmem] * len(blocks),
        out_specs=vmem,
        scratch_shapes=[pltpu.VMEM((req_dev * HEADS, HEAD_DIM), jnp.float32)],
        compiler_params=pltpu.CompilerParams(vmem_limit_bytes=16 * 2**20),
    )(*blocks)


def body(queries, keys, values, page_request, page_fill):
    count = lax.axis_size("seq")
    req_dev = queries.shape[0]
    page_request, page_fill = page_request[None], page_fill[None]
    by_xor = count <= 16
    if by_xor:
        pieces, late = gather_queries(queries, count), 3
        pieces = pieces[1:] + pieces[:1]
    else:
        whole, late = lax.all_gather(queries, "seq", axis=0), 0
        pieces = [whole[k] for k in range(count)]
    early = count - late
    own = attend(stage(pieces[:early]), pieces[early:], by_xor, keys, values, page_request, page_fill)
    _, given = lax.optimization_barrier((own, page_request))
    requests = [page_request] + [exchange(given, k, count) for k in range(1, LAYER)]
    across = exchange(own, 2, count)
    beside = exchange(own, 1, count)
    across, *requests = lax.optimization_barrier((across, *requests))
    rows = [own, beside, across, exchange(across, 1, count)]
    blocks = list(layer_merge(requests, rows, count // LAYER, req_dev))
    order = [k for k in range(count // LAYER - 1, 0, -1)]
    if len(order) == 3:
        order = [2, 3, 1]
    far = [exchange(blocks[k], LAYER * k, count) for k in order]
    return home_merge(blocks[:1] + far, req_dev)


def solution(mesh):
    placed = (
        P(("cell", "seq"), None),
        P(("cell", "seq"), None, None),
        P(("cell", "seq"), None, None),
        P(("cell", "seq")),
        P(("cell", "seq")),
    )
    return jax.shard_map(
        body, mesh=mesh, in_specs=placed, out_specs=P(("cell", "seq"), None), check_vma=False
    )
```

```python
import functools

import jax
import jax.numpy as jnp
from jax import lax
from jax.experimental import pallas as pl
from jax.experimental.pallas import tpu as pltpu
from jax.sharding import PartitionSpec as P

HEADS = 48
KV_HEADS = 8
HEAD_DIM = 128
GROUP = 6
LANES = 128
HALF = LANES // 2

FLOOR = -30000.0
LAYER = 4
STAGE_FLOPS = 20_000_000_000


def exchange(x, step, count):
    return lax.ppermute(x, "seq", [(i, i ^ step) for i in range(count)])


def gather_queries(queries, count):
    far = [4 * k for k in range(count // 4 - 1, 0, -1)]
    pieces = {0: queries}
    for step in far:
        pieces[step] = exchange(queries, step, count)
    for step in [0] + far[::-1]:
        pieces[step ^ 2] = exchange(pieces[step], 2, count)
    for step in list(pieces):
        pieces[step ^ 1] = exchange(pieces[step], 1, count)
    return [pieces[k] for k in range(count)]


def spread_out(block, rows, put):
    req_dev = block.shape[0]
    block = block[...].astype(jnp.float32)
    for h in range(HEADS):
        rows[req_dev * h : req_dev * (h + 1), :] = block[:, LANES * h : LANES * (h + 1)]
    for r in range(req_dev):
        put(r, rows[pl.ds(r, HEADS, stride=req_dev), :].astype(jnp.bfloat16))


def stage_kernel(*refs):
    blocks, (held, rows) = refs[:-2], refs[-2:]
    for k, block in enumerate(blocks):

        def put(r, tile, k=k):
            held[k, r] = tile

        spread_out(block, rows.at[k], put)


def stage(blocks):
    spec = pl.BlockSpec(memory_space=pltpu.VMEM)
    req_dev = blocks[0].shape[0]
    return pl.pallas_call(
        stage_kernel,
        name="stage",
        out_shape=jax.ShapeDtypeStruct((len(blocks), req_dev, HEADS, HEAD_DIM), jnp.bfloat16),
        in_specs=[spec] * len(blocks),
        out_specs=spec,
        scratch_shapes=[pltpu.VMEM((len(blocks), HEADS * req_dev, LANES), jnp.float32)],
        compiler_params=pltpu.CompilerParams(vmem_limit_bytes=16 * 2**20),
        cost_estimate=pl.CostEstimate(flops=STAGE_FLOPS, bytes_accessed=0, transcendentals=0),
    )(*blocks)


def split3(x):
    high = x.astype(jnp.bfloat16).astype(jnp.float32)
    middle = (x - high).astype(jnp.bfloat16).astype(jnp.float32)
    low = (x - high - middle).astype(jnp.bfloat16).astype(jnp.float32)
    return [high, middle, low]


def scalars(x):
    return [x[0, i] for i in range(x.shape[1])]


def divide(x, by):
    return x >> by.bit_length() - 1 if by & (by - 1) == 0 else x // by


def remainder(x, by):
    return x & (by - 1) if by & (by - 1) == 0 else x % by


def attend_kernel(late, by_xor, request_ref, fill_ref, held, *refs):
    late_refs, (keys, values, send, tail, rows, accs) = refs[:late], refs[late:]
    pages, page_len, _ = keys.shape
    early, req_dev, _, _ = held.shape
    me = lax.axis_index("seq") if by_xor else 0
    where = request_ref[...]
    block_at = divide(where, req_dev)
    if by_xor:
        block_at = remainder((block_at ^ me) + early + late - 1, early + late)
    block_at = scalars(block_at)
    row_at = scalars(remainder(where, req_dev))
    fill = scalars(fill_ref[...])
    for k in range(late):

        def put(r, tile, k=k):
            tail[k, r] = tile

        spread_out(late_refs[k], rows.at[k], put)
    lane = lax.broadcasted_iota(jnp.int32, (HEADS, LANES), 1)
    kv_of = lax.broadcasted_iota(jnp.int32, (HEADS, LANES), 0) // GROUP

    for p in range(pages):
        query = held[jnp.minimum(block_at[p], early - 1), row_at[p]]
        if late:
            last = tail[jnp.maximum(block_at[p] - early, 0), row_at[p]]
            query = jnp.where(block_at[p] < early, query, last)
        zero = jnp.zeros_like(query)
        wide = jnp.concatenate([jnp.where(kv_of == k, query, zero) for k in range(KV_HEADS)], axis=1)
        accs[p] = lax.dot_general(
            wide, keys[p], (((1,), (1,)), ((), ())), preferred_element_type=jnp.float32
        ) * HEAD_DIM ** (-0.5)

    heavy, totals = [], []
    stats = jnp.zeros((HEADS, LANES), jnp.float32)
    for p in range(pages):
        scores = accs[p]
        live = lax.broadcasted_iota(jnp.int32, (HEADS, page_len), 1) < fill[p]
        peak = jnp.max(jnp.where(live, scores, FLOOR), axis=1, keepdims=True)
        weights = jnp.where(live, jnp.exp(scores - peak), 0.0).astype(jnp.bfloat16)
        total = jnp.sum(weights.astype(jnp.float32), axis=1, keepdims=True)
        heavy.append(weights)
        totals.append(total)
        stats = jnp.where(lane == p, peak, stats)
        stats = jnp.where(lane == pages + p, total, stats)
    high, middle, low = split3(stats)
    stats = high + pltpu.roll(middle, 2 * pages, 1) + pltpu.roll(low, 4 * pages, 1)
    index = [divide(where, req_dev), remainder(where, req_dev)]
    index = jnp.concatenate(index + [jnp.zeros((1, LANES - 2 * pages), jnp.int32)], axis=1)
    index = pltpu.roll(index.astype(jnp.float32), 6 * pages, 1)
    inside = jnp.logical_and(lane >= 6 * pages, lane < 8 * pages)
    send[HEADS * pages :, :] = jnp.where(inside, index, stats).astype(send.dtype)

    for p in range(pages):
        mixed = lax.dot_general(
            heavy[p], values[p], (((1,), (0,)), ((), ())), preferred_element_type=jnp.float32
        )
        acc = mixed[:, :LANES]
        for k in range(1, KV_HEADS):
            acc = jnp.where(kv_of == k, mixed[:, LANES * k : LANES * (k + 1)], acc)
        send[HEADS * p : HEADS * (p + 1), :] = (acc / jnp.maximum(totals[p], 1.0)).astype(send.dtype)


def attend(held, late, by_xor, keys, values, page_request, page_fill):
    pages = keys.shape[0]
    req_dev = held.shape[1]
    vmem = pl.BlockSpec(memory_space=pltpu.VMEM)
    return pl.pallas_call(
        functools.partial(attend_kernel, len(late), by_xor),
        name="attend",
        out_shape=jax.ShapeDtypeStruct(((pages + 1) * HEADS, LANES), jnp.bfloat16),
        in_specs=[vmem] * (len(late) + 5),
        out_specs=vmem,
        scratch_shapes=[
            pltpu.VMEM((max(len(late), 1), req_dev, HEADS, HEAD_DIM), jnp.bfloat16),
            pltpu.VMEM((max(len(late), 1), HEADS * req_dev, LANES), jnp.float32),
            pltpu.VMEM((pages, HEADS, HEAD_DIM), jnp.float32),
        ],
        compiler_params=pltpu.CompilerParams(vmem_limit_bytes=32 * 2**20),
    )(page_request, page_fill, held, *late, keys, values)


def page_tables(blocks, slots, req_dev):
    pages = blocks[0].shape[0] // HEADS - 1
    me = lax.axis_index("seq")
    lane = lax.broadcasted_iota(jnp.int32, (HEADS, LANES), 1)
    peaks = jnp.full((HEADS, LANES), FLOOR, jnp.float32)
    totals = jnp.zeros((HEADS, LANES), jnp.float32)
    home = jnp.full((1, LANES), -1.0, jnp.float32)
    local = jnp.zeros((1, LANES), jnp.float32)
    for s, block in enumerate(blocks):
        stats = block[HEADS * pages :, :].astype(jnp.float32)
        whole = stats + pltpu.roll(stats, LANES - 2 * pages, 1) + pltpu.roll(stats, LANES - 4 * pages, 1)
        inside = jnp.logical_and(lane >= pages * s, lane < pages * (s + 1))
        peaks = jnp.where(inside, pltpu.roll(whole, (pages * s) % LANES, 1), peaks)
        totals = jnp.where(inside, pltpu.roll(whole, (pages * (s - 1)) % LANES, 1), totals)
        home = jnp.where(inside[:1], pltpu.roll(stats[:1], (pages * (s - 6)) % LANES, 1), home)
        local = jnp.where(inside[:1], pltpu.roll(stats[:1], (pages * (s - 7)) % LANES, 1), local)
    apart = home.astype(jnp.int32) ^ me
    mine = jnp.logical_and(home >= 0.0, remainder(apart, LAYER) == 0)
    where = jnp.where(mine, divide(apart, LAYER) * req_dev + local.astype(jnp.int32), slots)
    return peaks, totals, where


def layer_kernel(req_dev, *refs):
    blocks, outs, (sums, place, index, sem) = refs[:LAYER], refs[LAYER:-4], refs[-4:]
    pages = blocks[0].shape[0] // HEADS - 1
    slots = sums.shape[0] - 1
    lane = lax.broadcasted_iota(jnp.int32, (HEADS, LANES), 1)
    peaks, totals, where = page_tables(blocks, slots, req_dev)
    place[...] = where
    copy = pltpu.make_async_copy(place, index, sem)
    copy.start()
    sums[...] = jnp.zeros_like(sums)
    tops = jnp.zeros((HEADS, LANES), jnp.float32)
    slot_tops = jnp.full((HEADS, LANES), FLOOR, jnp.float32)
    for k in range(slots):
        top = jnp.max(jnp.where(where == k, peaks, FLOOR), axis=1, keepdims=True)
        tops = jnp.where(where == k, top, tops)
        slot_tops = jnp.where(lane == k, top, slot_tops)
    shares = jnp.where(where < slots, totals * jnp.exp(peaks - tops), 0.0)
    norms = jnp.ones((HEADS, LANES), jnp.float32)
    slot_wholes = jnp.zeros((HEADS, LANES), jnp.float32)
    for k in range(slots):
        whole = jnp.sum(jnp.where(where == k, shares, 0.0), axis=1, keepdims=True)
        slot_wholes = jnp.where(lane == k, whole, slot_wholes)
        norms = jnp.where(where == k, whole, norms)
    shares = shares / jnp.maximum(norms, 1.0)
    copy.wait()
    for i in range(LAYER * pages):
        s, p = divmod(i, pages)
        row = blocks[s][HEADS * p : HEADS * (p + 1), :].astype(jnp.float32)
        sums[index[0, i]] += row * shares[:, i : i + 1]

    pad = jnp.zeros((LANES - HEADS, LANES), jnp.float32)
    parts = []
    for table in (slot_tops, slot_wholes):
        flat = jnp.transpose(jnp.concatenate([table, pad], axis=0))
        parts += split3(flat[:slots])
    for k in range(len(outs)):
        for r in range(req_dev):
            outs[k][HEADS * r : HEADS * (r + 1), :] = sums[req_dev * k + r].astype(outs[k].dtype)
        lines = []
        for part in parts:
            part = part[req_dev * k : req_dev * (k + 1)]
            part = jnp.concatenate([part, jnp.zeros((8 - req_dev, LANES), jnp.float32)], axis=0)
            lines.append(part + pltpu.roll(pltpu.roll(part, 8 - req_dev // 2, 0), HALF, 1))
        tail = [line[: req_dev // 2] for line in lines]
        spare = outs[k].shape[0] - HEADS * req_dev - 3 * req_dev
        if spare:
            tail.append(jnp.zeros((spare, LANES), jnp.float32))
        outs[k][HEADS * req_dev :, :] = jnp.concatenate(tail, axis=0).astype(outs[k].dtype)


def layer_merge(own, count, homes, req_dev):
    vmem = pl.BlockSpec(memory_space=pltpu.VMEM)
    across = exchange(own, 2, count)
    blocks = [own, exchange(own, 1, count), across, exchange(across, 1, count)]
    height = HEADS * req_dev + -(-3 * req_dev // 8) * 8
    return pl.pallas_call(
        functools.partial(layer_kernel, req_dev),
        name="layer_merge",
        out_shape=[jax.ShapeDtypeStruct((height, LANES), jnp.bfloat16)] * homes,
        in_specs=[vmem] * LAYER,
        out_specs=[vmem] * homes,
        scratch_shapes=[
            pltpu.VMEM((homes * req_dev + 1, HEADS, HEAD_DIM), jnp.float32),
            pltpu.VMEM((1, LANES), jnp.int32),
            pltpu.SMEM((1, LANES), jnp.int32),
            pltpu.SemaphoreType.DMA,
        ],
        compiler_params=pltpu.CompilerParams(vmem_limit_bytes=16 * 2**20),
    )(*blocks)


def home_kernel(*refs):
    blocks, (out, accs) = refs[:-2], refs[-2:]
    req_dev = out.shape[0]
    half = req_dev // 2
    start = HEADS * req_dev
    peaks, totals = [], []
    for block in blocks:
        stats = block[start:, :].astype(jnp.float32)
        lines = [stats[half * i : half * (i + 1)] for i in range(6)]
        peaks.append(lines[0] + lines[1] + lines[2])
        totals.append(lines[3] + lines[4] + lines[5])
    top = functools.reduce(jnp.maximum, peaks)
    shares = [total * jnp.exp(peak - top) for peak, total in zip(peaks, totals)]
    whole = functools.reduce(jnp.add, shares)
    lane = lax.broadcasted_iota(jnp.int32, whole.shape, 1)
    whole = jnp.where(lane % HALF < HEADS, whole, 1.0)
    weights = [share / whole for share in shares]
    used = half * len(blocks)
    pad = jnp.zeros((LANES - used, LANES), jnp.float32)
    turned = jnp.transpose(jnp.concatenate(weights + [pad], axis=0))
    for r in range(req_dev):
        base = HALF * (r // half)
        acc = jnp.zeros((HEADS, HEAD_DIM), jnp.float32)
        for b, block in enumerate(blocks):
            column = half * b + r % half
            weight = turned[base : base + HEADS, column : column + 1]
            acc = acc + block[HEADS * r : HEADS * (r + 1), :].astype(jnp.float32) * weight
        accs[HEADS * r : HEADS * (r + 1), :] = acc
    for h in range(HEADS):
        out[:, LANES * h : LANES * (h + 1)] = accs[pl.ds(h, req_dev, stride=HEADS), :].astype(out.dtype)


def home_merge(blocks, req_dev):
    vmem = pl.BlockSpec(memory_space=pltpu.VMEM)
    return pl.pallas_call(
        home_kernel,
        name="home_merge",
        out_shape=jax.ShapeDtypeStruct((req_dev, HEADS * HEAD_DIM), jnp.bfloat16),
        in_specs=[vmem] * len(blocks),
        out_specs=vmem,
        scratch_shapes=[pltpu.VMEM((req_dev * HEADS, HEAD_DIM), jnp.float32)],
        compiler_params=pltpu.CompilerParams(vmem_limit_bytes=16 * 2**20),
    )(*blocks)


def body(queries, keys, values, page_request, page_fill):
    count = lax.axis_size("seq")
    req_dev = queries.shape[0]
    page_request, page_fill = page_request[None], page_fill[None]
    by_xor = count <= 16
    if by_xor:
        pieces, late = gather_queries(queries, count), 3
        pieces = pieces[1:] + pieces[:1]
    else:
        whole, late = lax.all_gather(queries, "seq", axis=0), 0
        pieces = [whole[k] for k in range(count)]
    early = count - late
    own = attend(stage(pieces[:early]), pieces[early:], by_xor, keys, values, page_request, page_fill)
    blocks = list(layer_merge(own, count, count // LAYER, req_dev))
    order = [k for k in range(count // LAYER - 1, 0, -1)]
    if len(order) == 3:
        order = [2, 3, 1]
    far = [exchange(blocks[k], LAYER * k, count) for k in order]
    return home_merge(blocks[:1] + far, req_dev)


def solution(mesh):
    placed = (
        P(("cell", "seq"), None),
        P(("cell", "seq"), None, None),
        P(("cell", "seq"), None, None),
        P(("cell", "seq")),
        P(("cell", "seq")),
    )
    return jax.shard_map(
        body, mesh=mesh, in_specs=placed, out_specs=P(("cell", "seq"), None), check_vma=False
    )
```

```python
import functools

import jax
import jax.numpy as jnp
from jax import lax
from jax.experimental import pallas as pl
from jax.experimental.pallas import tpu as pltpu
from jax.sharding import PartitionSpec as P


HEADS = 48
KV_HEADS = 8
HEAD_DIM = 128
GROUP = 6
LANES = 128
HALF = LANES // 2

FLOOR = -30000.0
LAYER = 4
STAGE_FLOPS = 20_000_000_000


def exchange(x, step, count):
    return lax.ppermute(x, "seq", [(i, i ^ step) for i in range(count)])


def gather_queries(queries, count):
    far = [4 * k for k in range(count // 4 - 1, 0, -1)]
    pieces = {0: queries}
    for step in far:
        pieces[step] = exchange(queries, step, count)
    for step in [0] + far[::-1]:
        pieces[step ^ 2] = exchange(pieces[step], 2, count)
    for step in list(pieces):
        pieces[step ^ 1] = exchange(pieces[step], 1, count)
    return [pieces[k] for k in range(count)]


def spread_out(block, rows, put):
    req_dev = block.shape[0]
    block = block[...].astype(jnp.float32)
    for h in range(HEADS):
        rows[req_dev * h : req_dev * (h + 1), :] = block[:, LANES * h : LANES * (h + 1)]
    for r in range(req_dev):
        put(r, rows[pl.ds(r, HEADS, stride=req_dev), :].astype(jnp.bfloat16))


def stage_kernel(*refs):
    blocks, (held, rows) = refs[:-2], refs[-2:]
    for k, block in enumerate(blocks):

        def put(r, tile, k=k):
            held[k, r] = tile

        spread_out(block, rows.at[k], put)


def stage(blocks):
    spec = pl.BlockSpec(memory_space=pltpu.VMEM)
    req_dev = blocks[0].shape[0]
    return pl.pallas_call(
        stage_kernel,
        name="stage",
        out_shape=jax.ShapeDtypeStruct((len(blocks), req_dev, HEADS, HEAD_DIM), jnp.bfloat16),
        in_specs=[spec] * len(blocks),
        out_specs=spec,
        scratch_shapes=[pltpu.VMEM((len(blocks), HEADS * req_dev, LANES), jnp.float32)],
        compiler_params=pltpu.CompilerParams(vmem_limit_bytes=16 * 2**20),
        cost_estimate=pl.CostEstimate(flops=STAGE_FLOPS, bytes_accessed=0, transcendentals=0),
    )(*blocks)


def split3(x):
    high = x.astype(jnp.bfloat16).astype(jnp.float32)
    middle = (x - high).astype(jnp.bfloat16).astype(jnp.float32)
    low = (x - high - middle).astype(jnp.bfloat16).astype(jnp.float32)
    return [high, middle, low]


def scalars(x):
    return [x[0, i] for i in range(x.shape[1])]


def divide(x, by):
    return x >> by.bit_length() - 1 if by & (by - 1) == 0 else x // by


def remainder(x, by):
    return x & (by - 1) if by & (by - 1) == 0 else x % by


def attend_kernel(late, by_xor, request_ref, fill_ref, held, *refs):
    late_refs, (keys, values, send, tail, rows, accs) = refs[:late], refs[late:]
    pages, page_len, _ = keys.shape
    early, req_dev, _, _ = held.shape
    me = lax.axis_index("seq") if by_xor else 0
    where = request_ref[...]
    block_at = divide(where, req_dev)
    if by_xor:
        block_at = remainder((block_at ^ me) + early + late - 1, early + late)
    block_at = scalars(block_at)
    row_at = scalars(remainder(where, req_dev))
    fill = scalars(fill_ref[...])
    for k in range(late):

        def put(r, tile, k=k):
            tail[k, r] = tile

        spread_out(late_refs[k], rows.at[k], put)
    lane = lax.broadcasted_iota(jnp.int32, (HEADS, LANES), 1)
    kv_of = lax.broadcasted_iota(jnp.int32, (HEADS, LANES), 0) // GROUP

    for p in range(pages):
        query = held[jnp.minimum(block_at[p], early - 1), row_at[p]]
        if late:
            last = tail[jnp.maximum(block_at[p] - early, 0), row_at[p]]
            query = jnp.where(block_at[p] < early, query, last)
        zero = jnp.zeros_like(query)
        wide = jnp.concatenate([jnp.where(kv_of == k, query, zero) for k in range(KV_HEADS)], axis=1)
        accs[p] = lax.dot_general(
            wide, keys[p], (((1,), (1,)), ((), ())), preferred_element_type=jnp.float32
        ) * HEAD_DIM ** (-0.5)

    heavy, totals = [], []
    stats = jnp.zeros((HEADS, LANES), jnp.float32)
    for p in range(pages):
        scores = accs[p]
        live = lax.broadcasted_iota(jnp.int32, (HEADS, page_len), 1) < fill[p]
        peak = jnp.max(jnp.where(live, scores, FLOOR), axis=1, keepdims=True)
        weights = jnp.where(live, jnp.exp(scores - peak), 0.0).astype(jnp.bfloat16)
        total = jnp.sum(weights.astype(jnp.float32), axis=1, keepdims=True)
        heavy.append(weights)
        totals.append(total)
        stats = jnp.where(lane == p, peak, stats)
        stats = jnp.where(lane == pages + p, total, stats)
    high, middle, low = split3(stats)
    stats = high + pltpu.roll(middle, 2 * pages, 1) + pltpu.roll(low, 4 * pages, 1)
    index = [divide(where, req_dev), remainder(where, req_dev)]
    index = jnp.concatenate(index + [jnp.zeros((1, LANES - 2 * pages), jnp.int32)], axis=1)
    index = pltpu.roll(index.astype(jnp.float32), 6 * pages, 1)
    inside = jnp.logical_and(lane >= 6 * pages, lane < 8 * pages)
    send[HEADS * pages :, :] = jnp.where(inside, index, stats).astype(send.dtype)

    for p in range(pages):
        mixed = lax.dot_general(
            heavy[p], values[p], (((1,), (0,)), ((), ())), preferred_element_type=jnp.float32
        )
        acc = mixed[:, :LANES]
        for k in range(1, KV_HEADS):
            acc = jnp.where(kv_of == k, mixed[:, LANES * k : LANES * (k + 1)], acc)
        send[HEADS * p : HEADS * (p + 1), :] = (acc / jnp.maximum(totals[p], 1.0)).astype(send.dtype)


def attend(held, late, by_xor, keys, values, page_request, page_fill):
    pages = keys.shape[0]
    req_dev = held.shape[1]
    vmem = pl.BlockSpec(memory_space=pltpu.VMEM)
    return pl.pallas_call(
        functools.partial(attend_kernel, len(late), by_xor),
        name="attend",
        out_shape=jax.ShapeDtypeStruct(((pages + 1) * HEADS, LANES), jnp.bfloat16),
        in_specs=[vmem] * (len(late) + 5),
        out_specs=vmem,
        scratch_shapes=[
            pltpu.VMEM((max(len(late), 1), req_dev, HEADS, HEAD_DIM), jnp.bfloat16),
            pltpu.VMEM((max(len(late), 1), HEADS * req_dev, LANES), jnp.float32),
            pltpu.VMEM((pages, HEADS, HEAD_DIM), jnp.float32),
        ],
        compiler_params=pltpu.CompilerParams(vmem_limit_bytes=32 * 2**20),
    )(page_request, page_fill, held, *late, keys, values)


def page_tables(blocks, slots, req_dev):
    pages = blocks[0].shape[0] // HEADS - 1
    me = lax.axis_index("seq")
    lane = lax.broadcasted_iota(jnp.int32, (HEADS, LANES), 1)
    peaks = jnp.full((HEADS, LANES), FLOOR, jnp.float32)
    totals = jnp.zeros((HEADS, LANES), jnp.float32)
    home = jnp.full((1, LANES), -1.0, jnp.float32)
    local = jnp.zeros((1, LANES), jnp.float32)
    for s, block in enumerate(blocks):
        stats = block[HEADS * pages :, :].astype(jnp.float32)
        whole = stats + pltpu.roll(stats, LANES - 2 * pages, 1) + pltpu.roll(stats, LANES - 4 * pages, 1)
        inside = jnp.logical_and(lane >= pages * s, lane < pages * (s + 1))
        peaks = jnp.where(inside, pltpu.roll(whole, (pages * s) % LANES, 1), peaks)
        totals = jnp.where(inside, pltpu.roll(whole, (pages * (s - 1)) % LANES, 1), totals)
        home = jnp.where(inside[:1], pltpu.roll(stats[:1], (pages * (s - 6)) % LANES, 1), home)
        local = jnp.where(inside[:1], pltpu.roll(stats[:1], (pages * (s - 7)) % LANES, 1), local)
    apart = home.astype(jnp.int32) ^ me
    mine = jnp.logical_and(home >= 0.0, remainder(apart, LAYER) == 0)
    where = jnp.where(mine, divide(apart, LAYER) * req_dev + local.astype(jnp.int32), slots)
    return peaks, totals, where


def layer_kernel(req_dev, *refs):
    blocks, outs, (sums, place, index, sem) = refs[:LAYER], refs[LAYER:-4], refs[-4:]
    pages = blocks[0].shape[0] // HEADS - 1
    slots = sums.shape[0] - 1
    lane = lax.broadcasted_iota(jnp.int32, (HEADS, LANES), 1)
    peaks, totals, where = page_tables(blocks, slots, req_dev)
    place[...] = where
    copy = pltpu.make_async_copy(place, index, sem)
    copy.start()
    sums[...] = jnp.zeros_like(sums)
    tops = jnp.zeros((HEADS, LANES), jnp.float32)
    slot_tops = jnp.full((HEADS, LANES), FLOOR, jnp.float32)
    for k in range(slots):
        top = jnp.max(jnp.where(where == k, peaks, FLOOR), axis=1, keepdims=True)
        tops = jnp.where(where == k, top, tops)
        slot_tops = jnp.where(lane == k, top, slot_tops)
    shares = jnp.where(where < slots, totals * jnp.exp(peaks - tops), 0.0)
    norms = jnp.ones((HEADS, LANES), jnp.float32)
    slot_wholes = jnp.zeros((HEADS, LANES), jnp.float32)
    for k in range(slots):
        whole = jnp.sum(jnp.where(where == k, shares, 0.0), axis=1, keepdims=True)
        slot_wholes = jnp.where(lane == k, whole, slot_wholes)
        norms = jnp.where(where == k, whole, norms)
    shares = shares / jnp.maximum(norms, 1.0)
    copy.wait()
    for i in range(LAYER * pages):
        s, p = divmod(i, pages)
        row = blocks[s][HEADS * p : HEADS * (p + 1), :].astype(jnp.float32)
        sums[index[0, i]] += row * shares[:, i : i + 1]

    pad = jnp.zeros((LANES - HEADS, LANES), jnp.float32)
    parts = []
    for table in (slot_tops, slot_wholes):
        flat = jnp.transpose(jnp.concatenate([table, pad], axis=0))
        parts += split3(flat[:slots])
    for k in range(len(outs)):
        for r in range(req_dev):
            outs[k][HEADS * r : HEADS * (r + 1), :] = sums[req_dev * k + r].astype(outs[k].dtype)
        lines = []
        for part in parts:
            part = part[req_dev * k : req_dev * (k + 1)]
            part = jnp.concatenate([part, jnp.zeros((8 - req_dev, LANES), jnp.float32)], axis=0)
            lines.append(part + pltpu.roll(pltpu.roll(part, 8 - req_dev // 2, 0), HALF, 1))
        tail = [line[: req_dev // 2] for line in lines]
        spare = outs[k].shape[0] - HEADS * req_dev - 3 * req_dev
        if spare:
            tail.append(jnp.zeros((spare, LANES), jnp.float32))
        outs[k][HEADS * req_dev :, :] = jnp.concatenate(tail, axis=0).astype(outs[k].dtype)


def layer_merge(own, count, homes, req_dev):
    vmem = pl.BlockSpec(memory_space=pltpu.VMEM)
    across = exchange(own, 2, count)
    blocks = [own, exchange(own, 1, count), across, exchange(across, 1, count)]
    height = HEADS * req_dev + -(-3 * req_dev // 8) * 8
    return pl.pallas_call(
        functools.partial(layer_kernel, req_dev),
        name="layer_merge",
        out_shape=[jax.ShapeDtypeStruct((height, LANES), jnp.bfloat16)] * homes,
        in_specs=[vmem] * LAYER,
        out_specs=[vmem] * homes,
        scratch_shapes=[
            pltpu.VMEM((homes * req_dev + 1, HEADS, HEAD_DIM), jnp.float32),
            pltpu.VMEM((1, LANES), jnp.int32),
            pltpu.SMEM((1, LANES), jnp.int32),
            pltpu.SemaphoreType.DMA,
        ],
        compiler_params=pltpu.CompilerParams(vmem_limit_bytes=16 * 2**20),
    )(*blocks)


def home_kernel(*refs):
    blocks, (out, accs) = refs[:-2], refs[-2:]
    req_dev = out.shape[0]
    half = req_dev // 2
    start = HEADS * req_dev
    peaks, totals = [], []
    for block in blocks:
        stats = block[start:, :].astype(jnp.float32)
        lines = [stats[half * i : half * (i + 1)] for i in range(6)]
        peaks.append(lines[0] + lines[1] + lines[2])
        totals.append(lines[3] + lines[4] + lines[5])
    top = functools.reduce(jnp.maximum, peaks)
    shares = [total * jnp.exp(peak - top) for peak, total in zip(peaks, totals)]
    whole = functools.reduce(jnp.add, shares)
    lane = lax.broadcasted_iota(jnp.int32, whole.shape, 1)
    whole = jnp.where(lane % HALF < HEADS, whole, 1.0)
    weights = [share / whole for share in shares]
    used = half * len(blocks)
    pad = jnp.zeros((LANES - used, LANES), jnp.float32)
    turned = jnp.transpose(jnp.concatenate(weights + [pad], axis=0))
    for r in range(req_dev):
        base = HALF * (r // half)
        acc = jnp.zeros((HEADS, HEAD_DIM), jnp.float32)
        for b, block in enumerate(blocks):
            column = half * b + r % half
            weight = turned[base : base + HEADS, column : column + 1]
            acc = acc + block[HEADS * r : HEADS * (r + 1), :].astype(jnp.float32) * weight
        accs[HEADS * r : HEADS * (r + 1), :] = acc
    for h in range(HEADS):
        out[:, LANES * h : LANES * (h + 1)] = accs[pl.ds(h, req_dev, stride=HEADS), :].astype(out.dtype)


def home_merge(blocks, req_dev):
    vmem = pl.BlockSpec(memory_space=pltpu.VMEM)
    return pl.pallas_call(
        home_kernel,
        name="home_merge",
        out_shape=jax.ShapeDtypeStruct((req_dev, HEADS * HEAD_DIM), jnp.bfloat16),
        in_specs=[vmem] * len(blocks),
        out_specs=vmem,
        scratch_shapes=[pltpu.VMEM((req_dev * HEADS, HEAD_DIM), jnp.float32)],
        compiler_params=pltpu.CompilerParams(vmem_limit_bytes=16 * 2**20),
    )(*blocks)


def steps(queries, keys, values, page_request, page_fill):
    count = lax.axis_size("seq")
    req_dev = queries.shape[0]
    page_request, page_fill = page_request[None], page_fill[None]
    by_xor = count <= 16
    if by_xor:
        pieces, late = gather_queries(queries, count), 3
        pieces = pieces[1:] + pieces[:1]
    else:
        whole, late = lax.all_gather(queries, "seq", axis=0), 0
        pieces = [whole[k] for k in range(count)]
    early = count - late
    own = attend(stage(pieces[:early]), pieces[early:], by_xor, keys, values, page_request, page_fill)
    blocks = list(layer_merge(own, count, count // LAYER, req_dev))
    order = [k for k in range(count // LAYER - 1, 0, -1)]
    if len(order) == 3:
        order = [2, 3, 1]
    far = [exchange(blocks[k], LAYER * k, count) for k in order]
    return home_merge(blocks[:1] + far, req_dev)


def solution(mesh):
    placed = (
        P(("cell", "seq"), None),
        P(("cell", "seq"), None, None),
        P(("cell", "seq"), None, None),
        P(("cell", "seq")),
        P(("cell", "seq")),
    )
    return jax.shard_map(steps, mesh=mesh, in_specs=placed, out_specs=P(("cell", "seq"), None), check_vma=False)
```

```python
import functools

import jax
import jax.numpy as jnp
from jax import lax
from jax.experimental import pallas as pl
from jax.experimental.pallas import tpu as pltpu
from jax.sharding import PartitionSpec as P


HEADS = 48
KV_HEADS = 8
HEAD_DIM = 128
GROUP = 6
LANES = 128
HALF = LANES // 2

FLOOR = -30000.0
LAYER = 4
STAGE_FLOPS = 20_000_000_000


def exchange(x, step, count):
    return lax.ppermute(x, "seq", [(i, i ^ step) for i in range(count)])


def gather_queries(queries, count):
    far = [4 * k for k in range(count // 4 - 1, 0, -1)]
    pieces = {0: queries}
    for step in far:
        pieces[step] = exchange(queries, step, count)
    for step in [0] + far[::-1]:
        pieces[step ^ 2] = exchange(pieces[step], 2, count)
    for step in list(pieces):
        pieces[step ^ 1] = exchange(pieces[step], 1, count)
    return [pieces[k] for k in range(count)]


def spread_out(block, rows, put):
    req_dev = block.shape[0]
    block = block[...].astype(jnp.float32)
    for h in range(HEADS):
        rows[req_dev * h : req_dev * (h + 1), :] = block[:, LANES * h : LANES * (h + 1)]
    for r in range(req_dev):
        put(r, rows[pl.ds(r, HEADS, stride=req_dev), :].astype(jnp.bfloat16))


def stage_kernel(*refs):
    blocks, (held, rows) = refs[:-2], refs[-2:]
    for k, block in enumerate(blocks):

        def put(r, tile, k=k):
            held[k, r] = tile

        spread_out(block, rows.at[k], put)


def stage(blocks):
    spec = pl.BlockSpec(memory_space=pltpu.VMEM)
    req_dev = blocks[0].shape[0]
    return pl.pallas_call(
        stage_kernel,
        name="stage",
        out_shape=jax.ShapeDtypeStruct((len(blocks), req_dev, HEADS, HEAD_DIM), jnp.bfloat16),
        in_specs=[spec] * len(blocks),
        out_specs=spec,
        scratch_shapes=[pltpu.VMEM((len(blocks), HEADS * req_dev, LANES), jnp.float32)],
        compiler_params=pltpu.CompilerParams(vmem_limit_bytes=16 * 2**20),
        cost_estimate=pl.CostEstimate(flops=STAGE_FLOPS, bytes_accessed=0, transcendentals=0),
    )(*blocks)


def split3(x):
    high = x.astype(jnp.bfloat16).astype(jnp.float32)
    middle = (x - high).astype(jnp.bfloat16).astype(jnp.float32)
    low = (x - high - middle).astype(jnp.bfloat16).astype(jnp.float32)
    return [high, middle, low]


def scalars(x):
    return [x[0, i] for i in range(x.shape[1])]


def divide(x, by):
    return x >> by.bit_length() - 1 if by & (by - 1) == 0 else x // by


def remainder(x, by):
    return x & (by - 1) if by & (by - 1) == 0 else x % by


def attend_kernel(late, by_xor, request_ref, fill_ref, held, *refs):
    late_refs, (keys, values, send, tail, rows, accs) = refs[:late], refs[late:]
    pages, page_len, _ = keys.shape
    early, req_dev, _, _ = held.shape
    me = lax.axis_index("seq") if by_xor else 0
    where = request_ref[...]
    block_at = divide(where, req_dev)
    if by_xor:
        block_at = remainder((block_at ^ me) + early + late - 1, early + late)
    block_at = scalars(block_at)
    row_at = scalars(remainder(where, req_dev))
    fill = scalars(fill_ref[...])
    for k in range(late):

        def put(r, tile, k=k):
            tail[k, r] = tile

        spread_out(late_refs[k], rows.at[k], put)
    lane = lax.broadcasted_iota(jnp.int32, (HEADS, LANES), 1)
    kv_of = lax.broadcasted_iota(jnp.int32, (HEADS, LANES), 0) // GROUP

    for p in range(pages):
        query = held[jnp.minimum(block_at[p], early - 1), row_at[p]]
        if late:
            last = tail[jnp.maximum(block_at[p] - early, 0), row_at[p]]
            query = jnp.where(block_at[p] < early, query, last)
        zero = jnp.zeros_like(query)
        wide = jnp.concatenate([jnp.where(kv_of == k, query, zero) for k in range(KV_HEADS)], axis=1)
        accs[p] = lax.dot_general(
            wide, keys[p], (((1,), (1,)), ((), ())), preferred_element_type=jnp.float32
        ) * HEAD_DIM ** (-0.5)

    heavy, totals = [], []
    stats = jnp.zeros((HEADS, LANES), jnp.float32)
    for p in range(pages):
        scores = accs[p]
        live = lax.broadcasted_iota(jnp.int32, (HEADS, page_len), 1) < fill[p]
        peak = jnp.max(jnp.where(live, scores, FLOOR), axis=1, keepdims=True)
        weights = jnp.where(live, jnp.exp(scores - peak), 0.0).astype(jnp.bfloat16)
        total = jnp.sum(weights.astype(jnp.float32), axis=1, keepdims=True)
        heavy.append(weights)
        totals.append(total)
        stats = jnp.where(lane == p, peak, stats)
        stats = jnp.where(lane == pages + p, total, stats)
    high, middle, low = split3(stats)
    stats = high + pltpu.roll(middle, 2 * pages, 1) + pltpu.roll(low, 4 * pages, 1)
    index = [divide(where, req_dev), remainder(where, req_dev)]
    index = jnp.concatenate(index + [jnp.zeros((1, LANES - 2 * pages), jnp.int32)], axis=1)
    index = pltpu.roll(index.astype(jnp.float32), 6 * pages, 1)
    inside = jnp.logical_and(lane >= 6 * pages, lane < 8 * pages)
    stats = jnp.where(inside, index, stats)
    stats = stats[: HEADS // 2] + pltpu.roll(stats[HEADS // 2 :], HALF, 1)
    send[HEADS * pages :, :] = stats.astype(send.dtype)

    for p in range(pages):
        mixed = lax.dot_general(
            heavy[p], values[p], (((1,), (0,)), ((), ())), preferred_element_type=jnp.float32
        )
        acc = mixed[:, :LANES]
        for k in range(1, KV_HEADS):
            acc = jnp.where(kv_of == k, mixed[:, LANES * k : LANES * (k + 1)], acc)
        send[HEADS * p : HEADS * (p + 1), :] = (acc / jnp.maximum(totals[p], 1.0)).astype(send.dtype)


def attend(held, late, by_xor, keys, values, page_request, page_fill):
    pages = keys.shape[0]
    req_dev = held.shape[1]
    vmem = pl.BlockSpec(memory_space=pltpu.VMEM)
    return pl.pallas_call(
        functools.partial(attend_kernel, len(late), by_xor),
        name="attend",
        out_shape=jax.ShapeDtypeStruct((pages * HEADS + HEADS // 2, LANES), jnp.bfloat16),
        in_specs=[vmem] * (len(late) + 5),
        out_specs=vmem,
        scratch_shapes=[
            pltpu.VMEM((max(len(late), 1), req_dev, HEADS, HEAD_DIM), jnp.bfloat16),
            pltpu.VMEM((max(len(late), 1), HEADS * req_dev, LANES), jnp.float32),
            pltpu.VMEM((pages, HEADS, HEAD_DIM), jnp.float32),
        ],
        compiler_params=pltpu.CompilerParams(vmem_limit_bytes=32 * 2**20),
    )(page_request, page_fill, held, *late, keys, values)


def page_tables(blocks, slots, req_dev):
    pages = blocks[0].shape[0] // HEADS
    me = lax.axis_index("seq")
    lane = lax.broadcasted_iota(jnp.int32, (HEADS, LANES), 1)
    peaks = jnp.full((HEADS, LANES), FLOOR, jnp.float32)
    totals = jnp.zeros((HEADS, LANES), jnp.float32)
    home = jnp.full((1, LANES), -1.0, jnp.float32)
    local = jnp.zeros((1, LANES), jnp.float32)
    for s, block in enumerate(blocks):
        stats = block[HEADS * pages :, :].astype(jnp.float32)
        stats = jnp.concatenate([stats, pltpu.roll(stats, HALF, 1)], axis=0)
        whole = stats + pltpu.roll(stats, LANES - 2 * pages, 1) + pltpu.roll(stats, LANES - 4 * pages, 1)
        inside = jnp.logical_and(lane >= pages * s, lane < pages * (s + 1))
        peaks = jnp.where(inside, pltpu.roll(whole, (pages * s) % LANES, 1), peaks)
        totals = jnp.where(inside, pltpu.roll(whole, (pages * (s - 1)) % LANES, 1), totals)
        home = jnp.where(inside[:1], pltpu.roll(stats[:1], (pages * (s - 6)) % LANES, 1), home)
        local = jnp.where(inside[:1], pltpu.roll(stats[:1], (pages * (s - 7)) % LANES, 1), local)
    apart = home.astype(jnp.int32) ^ me
    mine = jnp.logical_and(home >= 0.0, remainder(apart, LAYER) == 0)
    where = jnp.where(mine, divide(apart, LAYER) * req_dev + local.astype(jnp.int32), slots)
    return peaks, totals, where


def layer_kernel(req_dev, *refs):
    blocks, outs, (sums, place, index, sem) = refs[:LAYER], refs[LAYER:-4], refs[-4:]
    pages = blocks[0].shape[0] // HEADS
    slots = sums.shape[0] - 1
    lane = lax.broadcasted_iota(jnp.int32, (HEADS, LANES), 1)
    peaks, totals, where = page_tables(blocks, slots, req_dev)
    place[...] = where
    copy = pltpu.make_async_copy(place, index, sem)
    copy.start()
    sums[...] = jnp.zeros_like(sums)
    tops = jnp.zeros((HEADS, LANES), jnp.float32)
    slot_tops = jnp.full((HEADS, LANES), FLOOR, jnp.float32)
    for k in range(slots):
        top = jnp.max(jnp.where(where == k, peaks, FLOOR), axis=1, keepdims=True)
        tops = jnp.where(where == k, top, tops)
        slot_tops = jnp.where(lane == k, top, slot_tops)
    shares = jnp.where(where < slots, totals * jnp.exp(peaks - tops), 0.0)
    norms = jnp.ones((HEADS, LANES), jnp.float32)
    slot_wholes = jnp.zeros((HEADS, LANES), jnp.float32)
    for k in range(slots):
        whole = jnp.sum(jnp.where(where == k, shares, 0.0), axis=1, keepdims=True)
        slot_wholes = jnp.where(lane == k, whole, slot_wholes)
        norms = jnp.where(where == k, whole, norms)
    shares = shares / jnp.maximum(norms, 1.0)
    copy.wait()
    for i in range(LAYER * pages):
        s, p = divmod(i, pages)
        row = blocks[s][HEADS * p : HEADS * (p + 1), :].astype(jnp.float32)
        sums[index[0, i]] += row * shares[:, i : i + 1]

    pad = jnp.zeros((LANES - HEADS, LANES), jnp.float32)
    parts = []
    for table in (slot_tops, slot_wholes):
        flat = jnp.transpose(jnp.concatenate([table, pad], axis=0))
        parts += split3(flat[:slots])
    for k in range(len(outs)):
        for r in range(req_dev):
            outs[k][HEADS * r : HEADS * (r + 1), :] = sums[req_dev * k + r].astype(outs[k].dtype)
        lines = []
        for part in parts:
            part = part[req_dev * k : req_dev * (k + 1)]
            part = jnp.concatenate([part, jnp.zeros((8 - req_dev, LANES), jnp.float32)], axis=0)
            lines.append(part + pltpu.roll(pltpu.roll(part, 8 - req_dev // 2, 0), HALF, 1))
        tail = [line[: req_dev // 2] for line in lines]
        spare = outs[k].shape[0] - HEADS * req_dev - 3 * req_dev
        if spare:
            tail.append(jnp.zeros((spare, LANES), jnp.float32))
        outs[k][HEADS * req_dev :, :] = jnp.concatenate(tail, axis=0).astype(outs[k].dtype)


def layer_merge(own, count, homes, req_dev):
    vmem = pl.BlockSpec(memory_space=pltpu.VMEM)
    across = exchange(own, 2, count)
    blocks = [own, exchange(own, 1, count), across, exchange(across, 1, count)]
    height = HEADS * req_dev + -(-3 * req_dev // 8) * 8
    return pl.pallas_call(
        functools.partial(layer_kernel, req_dev),
        name="layer_merge",
        out_shape=[jax.ShapeDtypeStruct((height, LANES), jnp.bfloat16)] * homes,
        in_specs=[vmem] * LAYER,
        out_specs=[vmem] * homes,
        scratch_shapes=[
            pltpu.VMEM((homes * req_dev + 1, HEADS, HEAD_DIM), jnp.float32),
            pltpu.VMEM((1, LANES), jnp.int32),
            pltpu.SMEM((1, LANES), jnp.int32),
            pltpu.SemaphoreType.DMA,
        ],
        compiler_params=pltpu.CompilerParams(vmem_limit_bytes=16 * 2**20),
    )(*blocks)


def home_kernel(*refs):
    blocks, (out, accs) = refs[:-2], refs[-2:]
    req_dev = out.shape[0]
    half = req_dev // 2
    start = HEADS * req_dev
    peaks, totals = [], []
    for block in blocks:
        stats = block[start:, :].astype(jnp.float32)
        lines = [stats[half * i : half * (i + 1)] for i in range(6)]
        peaks.append(lines[0] + lines[1] + lines[2])
        totals.append(lines[3] + lines[4] + lines[5])
    top = functools.reduce(jnp.maximum, peaks)
    shares = [total * jnp.exp(peak - top) for peak, total in zip(peaks, totals)]
    whole = functools.reduce(jnp.add, shares)
    lane = lax.broadcasted_iota(jnp.int32, whole.shape, 1)
    whole = jnp.where(lane % HALF < HEADS, whole, 1.0)
    weights = [share / whole for share in shares]
    used = half * len(blocks)
    pad = jnp.zeros((LANES - used, LANES), jnp.float32)
    turned = jnp.transpose(jnp.concatenate(weights + [pad], axis=0))
    for r in range(req_dev):
        base = HALF * (r // half)
        acc = jnp.zeros((HEADS, HEAD_DIM), jnp.float32)
        for b, block in enumerate(blocks):
            column = half * b + r % half
            weight = turned[base : base + HEADS, column : column + 1]
            acc = acc + block[HEADS * r : HEADS * (r + 1), :].astype(jnp.float32) * weight
        accs[HEADS * r : HEADS * (r + 1), :] = acc
    for h in range(HEADS):
        out[:, LANES * h : LANES * (h + 1)] = accs[pl.ds(h, req_dev, stride=HEADS), :].astype(out.dtype)


def home_merge(blocks, req_dev):
    vmem = pl.BlockSpec(memory_space=pltpu.VMEM)
    return pl.pallas_call(
        home_kernel,
        name="home_merge",
        out_shape=jax.ShapeDtypeStruct((req_dev, HEADS * HEAD_DIM), jnp.bfloat16),
        in_specs=[vmem] * len(blocks),
        out_specs=vmem,
        scratch_shapes=[pltpu.VMEM((req_dev * HEADS, HEAD_DIM), jnp.float32)],
        compiler_params=pltpu.CompilerParams(vmem_limit_bytes=16 * 2**20),
    )(*blocks)


def steps(queries, keys, values, page_request, page_fill):
    count = lax.axis_size("seq")
    req_dev = queries.shape[0]
    page_request, page_fill = page_request[None], page_fill[None]
    by_xor = count <= 16
    if by_xor:
        pieces, late = gather_queries(queries, count), 3
        pieces = pieces[1:] + pieces[:1]
    else:
        whole, late = lax.all_gather(queries, "seq", axis=0), 0
        pieces = [whole[k] for k in range(count)]
    early = count - late
    own = attend(stage(pieces[:early]), pieces[early:], by_xor, keys, values, page_request, page_fill)
    blocks = list(layer_merge(own, count, count // LAYER, req_dev))
    order = [k for k in range(count // LAYER - 1, 0, -1)]
    if len(order) == 3:
        order = [2, 3, 1]
    far = [exchange(blocks[k], LAYER * k, count) for k in order]
    return home_merge(blocks[:1] + far, req_dev)


def solution(mesh):
    placed = (
        P(("cell", "seq"), None),
        P(("cell", "seq"), None, None),
        P(("cell", "seq"), None, None),
        P(("cell", "seq")),
        P(("cell", "seq")),
    )
    return jax.shard_map(steps, mesh=mesh, in_specs=placed, out_specs=P(("cell", "seq"), None), check_vma=False)
```
